512 devices in a mesh: band: 16 (over x, z_hi), fft: 32 (over y, z_lo, core).
Axes of the slice: x: 4, y: 8, z: 8 (z_hi: 4, z_lo: 2; z = z_hi * 2 + z_lo), core: 2. Of those that a mesh axis runs over, the one named last changes fastest.
Arguments:
- wave: float32 [2, 32, 128, 128, 128], P(None, 'band', 'fft'), may hold values from -6 to 6
- previous: float32 [2, 32, 128, 128, 128], P(None, 'band', 'fft'), may hold values from -6 to 6
- potential: float32 [128, 128, 128], P('band', 'fft'), may hold values from -1.5 to 1.5
- column_extent: int32 [128, 128], P('fft'), may hold values from -1 to 31, as said below
- metric: float32 [3], replicated, may hold values from 0.5 to 2
- center: float32 [1], replicated, may hold values from 0.5 to 2
- halfwidth: float32 [1], replicated, may hold values from 1 to 3
Outputs:
- filtered: float32 [2, 32, 128, 128, 128], P(None, 'band', 'fft')
The draws below stay inside these ranges and needn't reach their ends.
Inputs may be any that keep to these rules, and one draw needn't show every extreme that they name: `column_extent`: every entry is -1 where |s(gx)| >= 32 or |s(gy)| >= 32, with s the signed index of the steps. Some column reaches the maximum.
All inputs are finite; a program needn't handle non-finite values.
Results may differ from the reference program's by a relative error of at most 0.00005.
Values sent between devices are 32-bit elements; how exact they have to be, the bound alone decides.
A program may use at most 64 MiB of HBM per device.

```python
import math
import jax
import jax.numpy as jnp
from jax import lax

NX = 128
NY = 128
NZ = 128
BANDS = 32


def draw_column_extent(key, part):
    first_key, second_key = jax.random.split(key, 2)
    weights = jax.random.randint(first_key, (3,), 1, 5).astype(jnp.int32)
    largest = NZ // 4 - 1
    base_room = weights[2] * largest * largest
    radius_sq = base_room + jax.random.randint(second_key, (), 0, 1024).astype(jnp.int32) * (base_room // 1024 + 1)
    index_x = jnp.arange(NX, dtype=jnp.int32)
    index_y = jnp.arange(NY, dtype=jnp.int32)
    signed_x = jnp.where(index_x < NX // 2, index_x, index_x - NX)
    signed_y = jnp.where(index_y < NY // 2, index_y, index_y - NY)
    room_left = radius_sq - weights[0] * signed_x[:, None] ** 2 - weights[1] * signed_y[None, :] ** 2
    heights = jnp.arange(largest + 1, dtype=jnp.int32)
    counted = jnp.sum((weights[2] * heights[None, None, :] ** 2 <= room_left[:, :, None]).astype(jnp.int32), axis=2) - 1
    in_box = (jnp.abs(signed_x)[:, None] < NX // 4) & (jnp.abs(signed_y)[None, :] < NY // 4)
    return jnp.where(in_box, counted, -1).astype(jnp.int32)


def shard_levels(key, dims, shards, smallest, high):
    factor_of, own = 1.0, jax.random.fold_in(key, 6)
    for dim, blocks in shards:
        steps = jnp.exp(jax.random.uniform(jax.random.fold_in(own, dim), (blocks,), jnp.float32, smallest / len(shards), high / len(shards)))
        factor_of = factor_of * jnp.repeat(steps, dims[dim] // blocks).reshape([-1 if axis == dim else 1 for axis in range(len(dims))])
    return factor_of


def noise(rng, extent, deviation, bound, cuts=(), kind=jnp.bfloat16):
    values = jax.random.normal(rng, extent, jnp.float32) * deviation
    if len(cuts) > 0:
        values = shard_levels(rng, extent, cuts, -0.22, 0.18) * values
    return jnp.clip(values, min=-bound, max=bound).astype(kind)


def setup_inputs(seed: int = 0) -> dict:
    keys = jax.random.split(jax.random.key(seed), 8)
    return {
        "wave": noise(keys[0], (2, BANDS, NX, NZ, NY), 1.0, 6.0, ((1, 16), (2, 32)), jnp.float32),
        "previous": noise(keys[1], (2, BANDS, NX, NZ, NY), 1.0, 6.0, ((1, 16), (2, 32)), jnp.float32),
        "potential": jnp.clip(jax.random.uniform(keys[2], (NX, NZ, NY), jnp.float32, -1.5, 1.5) * shard_levels(keys[2], (NX, NZ, NY), ((0, 16), (1, 32)), -0.4, 0.0), -1.5, 1.5),
        "column_extent": draw_column_extent(jax.random.fold_in(keys[7], 71), 0),
        "metric": jnp.clip(jnp.exp(jax.random.uniform(keys[4], (3,), jnp.float32, math.log(0.5), math.log(2.0))), 0.5, 2.0),
        "center": jnp.clip(jax.random.uniform(keys[5], (1,), jnp.float32, 0.5, 2.0), 0.5, 2.0),
        "halfwidth": jnp.clip(jnp.exp(jax.random.uniform(keys[6], (1,), jnp.float32, math.log(1.0), math.log(3.0))), 1.0, 3.0),
    }


def signed(length):
    indices = jnp.arange(length, dtype=jnp.int32)
    return jnp.where(indices < length // 2, indices, indices - length)


def reference(wave, previous, potential, column_extent, metric, center, halfwidth):
    keep_mask = (jnp.abs(signed(NZ))[None, :, None] <= column_extent[:, None, :]).astype(jnp.float32)
    two_pi = 2.0 * math.pi
    kinetic_x = (two_pi * signed(NX).astype(jnp.float32) / NX) ** 2
    kinetic_y = (two_pi * signed(NY).astype(jnp.float32) / NY) ** 2
    kinetic_z = (two_pi * signed(NZ).astype(jnp.float32) / NZ) ** 2
    kinetic = 0.5 * (metric[0] * kinetic_x[:, None, None] + metric[2] * kinetic_z[None, :, None] + metric[1] * kinetic_y[None, None, :])
    cell_count = NX * NY * NZ
    factor = 2.0 / halfwidth[0]

    def one_band(pieces):
        real_in, imag_in, real_prev, imag_prev = pieces
        coefficient = (real_in + 1j * imag_in) * keep_mask
        real_space = jnp.fft.ifftn(coefficient) * cell_count
        potential_term = jnp.fft.fftn(potential * real_space) / cell_count
        applied = kinetic * coefficient + potential_term
        result = keep_mask * (factor * (applied - center[0] * coefficient) - (real_prev + 1j * imag_prev))
        return jnp.real(result).astype(jnp.float32), jnp.imag(result).astype(jnp.float32)

    real_out, imag_out = lax.map(one_band, (wave[0], wave[1], previous[0], previous[1]))
    return jnp.stack([real_out, imag_out])
```

```python
import functools
import math

import jax
import jax.numpy as jnp
import numpy as np
from jax import lax
from jax.experimental import pallas as pl
from jax.experimental.pallas import tpu as pltpu
from jax.sharding import PartitionSpec as P

N = 128
KEPT = 64
HALF = KEPT // 2
FFT = 32
ACTIVE = 16
BANDS = 2
MESH = pl.DeviceIdType.MESH


def kept_indices():
    return np.concatenate([np.arange(HALF), np.arange(N - HALF, N)])


def cos_sin(rows, cols):
    angles = (np.outer(rows, cols) % N) * (2.0 * math.pi / N)
    return np.cos(angles), np.sin(angles)


def split(table):
    high = table.astype(jnp.bfloat16)
    low = (table - high.astype(np.float64)).astype(jnp.bfloat16)
    return high, low


def stacked(cosine, sine):
    cos_high, cos_low = split(cosine)
    sin_high, sin_low = split(sine)
    zero = np.zeros_like(cos_low)
    return np.concatenate(
        [
            np.concatenate([cos_high, cos_high], axis=1),
            np.concatenate([sin_high, sin_high], axis=1),
            np.concatenate([cos_low, zero], axis=1),
            np.concatenate([sin_low, zero], axis=1),
        ],
        axis=0,
    )


def make_tables():
    grid = np.arange(N)
    kept = kept_indices()
    slots = np.arange(ACTIVE)
    first_gx = 4 * np.where(slots < ACTIVE // 2, slots, slots + FFT - ACTIVE)

    cosine, sine = cos_sin(grid, kept)
    base = np.concatenate([cosine, sine], axis=1).reshape(FFT, 4, 2 * KEPT)
    full = np.zeros((FFT, 2, 4, 2, 2 * KEPT))
    for q in range(2):
        full[:, q, :, q, :] = base
    inverse_z = np.concatenate(split(full.reshape(2 * N, 2 * N)), axis=1)

    lanes = np.arange(N)
    natural = (lanes < HALF) | (lanes >= N - HALF)
    gy = np.where(natural, lanes, (lanes + KEPT) % N)
    cosine, sine = cos_sin(gy, grid)
    pick = natural[:, None]
    table = np.concatenate([np.where(pick, cosine, -sine), np.where(pick, sine, cosine)], axis=1)
    high, low = split(table)
    inverse_y = np.concatenate([high, high, low], axis=0)

    order = (first_gx[None, :, None] + 2 * np.arange(2)[:, None, None] + np.arange(2)[None, None, :]).reshape(-1)
    cosine, sine = cos_sin(grid, order)
    cos_high, cos_low = split(cosine)
    sin_high, sin_low = split(sine)
    zero = np.zeros_like(cos_low)
    inverse_x = np.concatenate(
        [
            np.concatenate([cos_high, sin_high, cos_high, sin_high], axis=1),
            np.concatenate([cos_low, sin_low, zero, zero], axis=1),
        ],
        axis=0,
    )

    order = (np.arange(4)[:, None] + first_gx[None, :]).reshape(-1)
    cosine, sine = cos_sin(order, grid)
    forward_x = stacked(cosine / N, sine / N)

    cosine, sine = cos_sin(grid, gy)
    pick = natural[None, :]
    table = np.concatenate([np.where(pick, cosine, -sine), np.where(pick, sine, cosine)], axis=0) / N
    forward_y = np.concatenate(split(table), axis=1)

    cosine, sine = cos_sin(kept, grid)
    forward_z = stacked(cosine / N, sine / N)
    return [inverse_z, inverse_y, inverse_x, forward_x, forward_y, forward_z]


def halves(value):
    high = value.astype(jnp.bfloat16)
    low = (value - high.astype(jnp.float32)).astype(jnp.bfloat16)
    return high, low


def dot(left, right):
    return jnp.dot(left, right, preferred_element_type=jnp.float32)


def kernel(
    wave,
    previous,
    potential,
    extent,
    metric,
    center,
    halfwidth,
    iz_hbm,
    iy_hbm,
    ix_hbm,
    fx_hbm,
    fy_hbm,
    fz_hbm,
    out,
    wbuf,
    pbuf,
    vbuf,
    iz,
    iy,
    ix,
    fx,
    fy,
    fz,
    zhigh,
    zlow,
    sbuf,
    rbuf,
    yre,
    yim,
    qhigh,
    qlow,
    gbuf,
    hbuf,
    obuf,
    wsem,
    psem,
    tsem,
    lsem,
    osem,
    fsend,
    frecv,
    gsend,
    grecv,
    vsend,
    vrecv,
):
    me = lax.axis_index("fft")
    band = lax.axis_index("band")
    my_x, my_z = band // 4, band % 4
    active = jnp.logical_or(me < ACTIVE // 2, me >= FFT - ACTIVE // 2)
    slot = jnp.where(me < ACTIVE // 2, me, me - (FFT - ACTIVE))

    def peer_at(step):
        spot = step + jnp.where(step >= 28, 1, 0)
        k, i = spot // 4, spot % 4
        dy = 4 + (1 - 2 * (k % 2)) * ((k + 1) // 2)
        return ((me // 4 + dy) % 8) * 4 + (me + i) % 4

    load_v = pltpu.make_async_copy(potential, vbuf.at[pl.ds(pl.multiple_of(band * 32, 32), 32), :], lsem)
    load_v.start()
    table_refs = ((iz_hbm, iz), (iy_hbm, iy), (ix_hbm, ix), (fx_hbm, fx), (fy_hbm, fy), (fz_hbm, fz))
    table_copies = [pltpu.make_async_copy(a, b, tsem.at[i]) for i, (a, b) in enumerate(table_refs)]

    def wave_copies(b):
        return [
            pltpu.make_async_copy(
                wave.at[:, b, :, pl.ds(h * (N - HALF), HALF), :],
                wbuf.at[:, b, :, pl.ds(h * HALF, HALF), :],
                wsem.at[b, h],
            )
            for h in range(2)
        ]

    def previous_copies():
        return [
            pltpu.make_async_copy(
                previous.at[:, :, :, pl.ds(h * (N - HALF), HALF), :],
                pbuf.at[:, :, :, pl.ds(h * HALF, HALF), :],
                psem.at[h],
            )
            for h in range(2)
        ]

    @pl.when(active)
    def _():
        for b in range(BANDS):
            for copy in wave_copies(b):
                copy.start()

    for copy in table_copies:
        copy.start()

    barrier = pltpu.get_barrier_semaphore()

    def greet(step, carry):
        pl.semaphore_signal(barrier, inc=1, device_id={"fft": peer_at(step)}, device_id_type=MESH)
        return carry

    lax.fori_loop(0, FFT - 1, greet, 0)
    z_peers = [my_x * 4 + (my_z + d) % 4 for d in (2, 1, 3)]
    x_peers = [((my_x + d) % 4) * 4 + my_z for d in (2, 1, 3)]
    for peer in z_peers + x_peers:
        pl.semaphore_signal(barrier, inc=1, device_id={"band": peer}, device_id_type=MESH)

    @pl.when(active)
    def _():
        for copy in previous_copies():
            copy.start()

    row = lax.broadcasted_iota(jnp.int32, (KEPT, N), 0)
    lane = lax.broadcasted_iota(jnp.int32, (KEPT, N), 1)
    signed_gz = jnp.where(row < HALF, row, row - KEPT)
    signed_gy = jnp.where(lane < N // 2, lane, lane - N)
    turn = jnp.where(jnp.logical_or(lane < HALF, lane >= N - HALF), -1.0, 1.0).astype(jnp.float32)

    def keep_of(j):
        return (jnp.abs(signed_gz) <= extent[pl.ds(j, 1), :]).astype(jnp.float32)

    def to_planes(b):
        for copy in wave_copies(b):
            copy.wait()
        for p in range(2):
            for q in range(2):
                j = 2 * p + q
                keep = keep_of(j)
                packed = keep * wbuf[0, b, j] + pltpu.roll(keep * wbuf[1, b, j], KEPT, axis=1)
                turned = pltpu.roll(packed, KEPT, axis=1) * turn
                for t, part in enumerate((packed, turned)):
                    high, low = halves(part)
                    rows = slice((2 * q + t) * KEPT, (2 * q + t + 1) * KEPT)
                    zhigh[rows, p * N : (p + 1) * N] = high
                    zlow[rows, p * N : (p + 1) * N] = low
        sbuf[b] = (
            dot(iz[:, : 2 * N], zhigh[...]) + dot(iz[:, 2 * N :], zhigh[...]) + dot(iz[:, : 2 * N], zlow[...])
        )
        mine = sbuf[b, pl.ds(pl.multiple_of(me * 8, 8), 8), :]
        rbuf[b, pl.ds(pl.multiple_of(slot * 8, 8), 8), :] = mine

    def plane_copy(b, peer):
        return pltpu.make_async_remote_copy(
            src_ref=sbuf.at[b, pl.ds(pl.multiple_of(peer * 8, 8), 8), :],
            dst_ref=rbuf.at[b, pl.ds(pl.multiple_of(slot * 8, 8), 8), :],
            send_sem=fsend.at[b],
            recv_sem=frecv.at[b],
            device_id={"fft": peer},
            device_id_type=MESH,
        )

    def send_planes(b):
        def step(n, carry):
            plane_copy(b, peer_at(n)).start()
            return carry

        lax.fori_loop(0, FFT - 1, step, 0)

    def column_copy(b, peer):
        where = jnp.where(peer < ACTIVE // 2, peer, peer - (FFT - ACTIVE))
        return pltpu.make_async_remote_copy(
            src_ref=gbuf.at[b, pl.ds(pl.multiple_of(where * 16, 16), 16), :],
            dst_ref=hbuf.at[b, pl.ds(pl.multiple_of(me * 16, 16), 16), :],
            send_sem=gsend.at[b],
            recv_sem=grecv.at[b],
            device_id={"fft": peer},
            device_id_type=MESH,
        )

    def send_columns(b):
        def step(n, carry):
            peer = peer_at(n)

            @pl.when(jnp.logical_or(peer < ACTIVE // 2, peer >= FFT - ACTIVE // 2))
            def _():
                column_copy(b, peer).start()

            return carry

        lax.fori_loop(0, FFT - 1, step, 0)

    def awaited(ref, send, recv):
        return pltpu.make_async_remote_copy(
            src_ref=ref, dst_ref=ref, send_sem=send, recv_sem=recv, device_id={"fft": me}, device_id_type=MESH
        )

    def v_copy(start, rows, phase, peer):
        where = vbuf.at[pl.ds(pl.multiple_of(start, 32), rows), :]
        return pltpu.make_async_remote_copy(
            src_ref=where,
            dst_ref=where,
            send_sem=vsend.at[phase],
            recv_sem=vrecv.at[phase],
            device_id={"band": peer},
            device_id_type=MESH,
        )

    @pl.when(active)
    def _():
        table_copies[0].wait()
        to_planes(0)

    load_v.wait()
    pl.semaphore_wait(barrier, FFT - 1 + 6)

    for peer in z_peers:
        v_copy(band * 32, 32, 0, peer).start()

    @pl.when(active)
    def _():
        send_planes(0)
        to_planes(1)
        send_planes(1)
        obuf[...] = jnp.zeros_like(obuf)

    @pl.when(jnp.logical_not(active))
    def _():
        table_copies[0].wait()
        obuf[...] = jnp.zeros_like(obuf)
        for b in range(BANDS):
            pltpu.make_async_copy(obuf.at[:, b], out.at[:, b], osem.at[b]).start()

    awaited(vbuf.at[pl.ds(0, 96), :], vsend.at[0], vrecv.at[0]).wait_recv()
    for peer in x_peers:
        v_copy(my_x * 128, 128, 1, peer).start()

    for copy in table_copies[1:5]:
        copy.wait()

    for b in range(BANDS):

        @pl.when(active)
        def _():
            awaited(rbuf.at[b, pl.ds(0, 8 * (ACTIVE - 1)), :], fsend.at[b], frecv.at[b]).wait_recv()

        @pl.when(jnp.logical_not(active))
        def _():
            awaited(rbuf.at[b], fsend.at[b], frecv.at[b]).wait_recv()

        for p in range(2):
            high, low = halves(rbuf[b, :, p * N : (p + 1) * N])
            plane = dot(jnp.concatenate([high, low, high], axis=1), iy[...])
            yre[p * N : (p + 1) * N, :] = plane[:, :N]
            yim[p * N : (p + 1) * N, :] = plane[:, N:]
        if b == 0:
            awaited(vbuf.at[pl.ds(0, 384), :], vsend.at[1], vrecv.at[1]).wait_recv()
        for z in range(4):
            rh, rl = halves(yre[pl.ds(z, KEPT, stride=4), :])
            ih, il = halves(yim[pl.ds(z, KEPT, stride=4), :])
            right = jnp.concatenate(
                [
                    jnp.concatenate([rh, ih], axis=1),
                    jnp.concatenate([-ih, rh], axis=1),
                    jnp.concatenate([rl, il], axis=1),
                    jnp.concatenate([-il, rl], axis=1),
                ],
                axis=0,
            )
            field = dot(ix[...], right)
            field = field[:N] + field[N:]
            local_v = vbuf[pl.ds(z, N, stride=4), :]
            rh, rl = halves(field[:, :N] * local_v)
            ih, il = halves(field[:, N:] * local_v)
            right = jnp.concatenate(
                [jnp.concatenate([rh, ih], axis=1), jnp.concatenate([rl, il], axis=1)], axis=0
            )
            both = dot(fx[...], right)
            both = both[:N] + both[N:]
            cos_part, sin_part = both[:KEPT], both[KEPT:]
            high, low = halves(cos_part[:, :N] + sin_part[:, N:])
            qhigh[z * KEPT : (z + 1) * KEPT, :N] = high
            qlow[z * KEPT : (z + 1) * KEPT, :N] = low
            high, low = halves(cos_part[:, N:] - sin_part[:, :N])
            qhigh[z * KEPT : (z + 1) * KEPT, N:] = high
            qlow[z * KEPT : (z + 1) * KEPT, N:] = low
        wide = dot(qhigh[...], fy[...])
        packed = wide[:, :N] + wide[:, N:] + dot(qlow[...], fy[:, :N])
        for z in range(4):
            for j in range(4):
                gbuf[b, pl.ds(z * 4 + j, ACTIVE, stride=16), :] = packed[
                    z * KEPT + j * ACTIVE : z * KEPT + (j + 1) * ACTIVE
                ]

        @pl.when(active)
        def _():
            mine = gbuf[b, pl.ds(pl.multiple_of(slot * 16, 16), 16), :]
            hbuf[b, pl.ds(pl.multiple_of(me * 16, 16), 16), :] = mine

        send_columns(b)

    table_copies[5].wait()

    @pl.when(active)
    def _():
        for copy in previous_copies():
            copy.wait()
        step_z = (2.0 * math.pi / N) * signed_gz.astype(jnp.float32)
        step_y = (2.0 * math.pi / N) * signed_gy.astype(jnp.float32)
        plane_kinetic = metric[2] * (step_z * step_z) + metric[1] * (step_y * step_y)
        factor = jnp.full((1, 1), 2.0, jnp.float32) / jnp.full((1, 1), halfwidth[0], jnp.float32)
        middle = center[0]
        for b in range(BANDS):
            awaited(hbuf.at[b, pl.ds(0, 16 * (FFT - 1)), :], gsend.at[b], grecv.at[b]).wait_recv()
            for p in range(2):
                h0, l0 = halves(hbuf[b, pl.ds(2 * p, N, stride=4), :])
                h1, l1 = halves(hbuf[b, pl.ds(2 * p + 1, N, stride=4), :])
                right = jnp.concatenate(
                    [jnp.concatenate([h0, h1], axis=1), jnp.concatenate([l0, l1], axis=1)], axis=0
                )
                both = dot(fz[...], right)
                both = both[:N] + both[N:]
                for q in range(2):
                    j = 2 * p + q
                    cos_part = both[:KEPT, q * N : (q + 1) * N]
                    sin_part = both[KEPT:, q * N : (q + 1) * N]
                    applied = cos_part - turn * pltpu.roll(sin_part, KEPT, axis=1)
                    keep = keep_of(j)
                    gx = me * 4 + j
                    signed_gx = jnp.where(gx < N // 2, gx, gx - N).astype(jnp.float32)
                    step_x = (2.0 * math.pi / N) * signed_gx
                    kinetic = 0.5 * (metric[0] * (step_x * step_x) + plane_kinetic)
                    for t, term in enumerate((applied, pltpu.roll(applied, KEPT, axis=1))):
                        coefficient = keep * wbuf[t, b, j]
                        result = keep * (
                            factor * (kinetic * coefficient + term - middle * coefficient) - pbuf[t, b, j]
                        )
                        obuf[t, b, j, :HALF, :] = result[:HALF]
                        obuf[t, b, j, N - HALF :, :] = result[HALF:]
            pltpu.make_async_copy(obuf.at[:, b], out.at[:, b], osem.at[b]).start()

    @pl.when(active)
    def _():
        for b in range(BANDS):
            awaited(sbuf.at[b, pl.ds(0, 8 * (FFT - 1)), :], fsend.at[b], frecv.at[b]).wait_send()
            awaited(gbuf.at[b, pl.ds(0, 16 * (ACTIVE - 1)), :], gsend.at[b], grecv.at[b]).wait_send()

    @pl.when(jnp.logical_not(active))
    def _():
        for b in range(BANDS):
            awaited(gbuf.at[b], gsend.at[b], grecv.at[b]).wait_send()

    awaited(vbuf.at[pl.ds(0, 96), :], vsend.at[0], vrecv.at[0]).wait_send()
    awaited(vbuf.at[pl.ds(0, 384), :], vsend.at[1], vrecv.at[1]).wait_send()
    for b in range(BANDS):
        pltpu.make_async_copy(obuf.at[:, b], out.at[:, b], osem.at[b]).wait()


def local(tables, wave, previous, potential, column_extent, metric, center, halfwidth):
    any_spec = pl.BlockSpec(memory_space=pl.ANY)
    vmem_spec = pl.BlockSpec(memory_space=pltpu.VMEM)
    smem_spec = pl.BlockSpec(memory_space=pltpu.SMEM)
    f32, bf16 = jnp.float32, jnp.bfloat16
    dma = pltpu.SemaphoreType.DMA
    return pl.pallas_call(
        kernel,
        out_shape=jax.ShapeDtypeStruct(wave.shape, f32),
        in_specs=[any_spec, any_spec, any_spec, vmem_spec, smem_spec, smem_spec, smem_spec] + [any_spec] * 6,
        out_specs=any_spec,
        scratch_shapes=[
            pltpu.VMEM((2, BANDS, 4, KEPT, N), f32),
            pltpu.VMEM((2, BANDS, 4, KEPT, N), f32),
            pltpu.VMEM((4 * N, N), f32),
            *[pltpu.VMEM(table.shape, bf16) for table in tables],
            pltpu.VMEM((2 * N, 2 * N), bf16),
            pltpu.VMEM((2 * N, 2 * N), bf16),
            pltpu.VMEM((BANDS, 2 * N, 2 * N), f32),
            pltpu.VMEM((BANDS, N, 2 * N), f32),
            pltpu.VMEM((2 * N, N), f32),
            pltpu.VMEM((2 * N, N), f32),
            pltpu.VMEM((2 * N, 2 * N), bf16),
            pltpu.VMEM((2 * N, 2 * N), bf16),
            pltpu.VMEM((BANDS, 2 * N, N), f32),
            pltpu.VMEM((BANDS, 4 * N, N), f32),
            pltpu.VMEM((2, BANDS, 4, N, N), f32),
            dma((BANDS, 2)),
            dma((2,)),
            dma((6,)),
            dma,
            dma((BANDS,)),
            dma((BANDS,)),
            dma((BANDS,)),
            dma((BANDS,)),
            dma((BANDS,)),
            dma((2,)),
            dma((2,)),
        ],
        compiler_params=pltpu.CompilerParams(collective_id=0, has_side_effects=True),
    )(wave, previous, potential.reshape(32, N), column_extent, metric, center, halfwidth, *tables)


def solution(mesh):
    tables = [jnp.asarray(table) for table in make_tables()]
    in_specs = (
        P(None, "band", "fft", None, None),
        P(None, "band", "fft", None, None),
        P("band", "fft", None),
        P("fft", None),
        P(),
        P(),
        P(),
    )
    out_specs = P(None, "band", "fft", None, None)
    return jax.shard_map(
        functools.partial(local, tables), mesh=mesh, in_specs=in_specs, out_specs=out_specs, check_vma=False
    )
```

```python
import functools
import math

import jax
import jax.numpy as jnp
import numpy as np
from jax import lax
from jax.experimental import pallas as pl
from jax.experimental.pallas import tpu as pltpu
from jax.sharding import PartitionSpec as P

N = 128
KEPT = 64
HALF = KEPT // 2
FFT = 32
ACTIVE = 16
BANDS = 2
PLANES = 5
FEW = 3
MESH = pl.DeviceIdType.MESH


def kept_indices():
    return np.concatenate([np.arange(HALF), np.arange(N - HALF, N)])


def cos_sin(rows, cols):
    angles = (np.outer(rows, cols) % N) * (2.0 * math.pi / N)
    return np.cos(angles), np.sin(angles)


def split(table):
    high = table.astype(jnp.bfloat16)
    low = (table - high.astype(np.float64)).astype(jnp.bfloat16)
    return high, low


def stacked(cosine, sine):
    cos_high, cos_low = split(cosine)
    sin_high, sin_low = split(sine)
    zero = np.zeros_like(cos_low)
    return np.concatenate(
        [
            np.concatenate([cos_high, cos_high], axis=1),
            np.concatenate([sin_high, sin_high], axis=1),
            np.concatenate([cos_low, zero], axis=1),
            np.concatenate([sin_low, zero], axis=1),
        ],
        axis=0,
    )


def make_tables():
    grid = np.arange(N)
    kept = kept_indices()
    slots = np.arange(ACTIVE)
    first_gx = 4 * np.where(slots < ACTIVE // 2, slots, slots + FFT - ACTIVE)

    cosine, sine = cos_sin(grid, kept)
    high, low = split(np.concatenate([cosine, sine], axis=1))
    zero = np.zeros_like(low)
    inverse_z = np.concatenate([np.concatenate([high, high], axis=1), np.concatenate([low, zero], axis=1)], axis=0)

    lanes = np.arange(N)
    natural = (lanes < HALF) | (lanes >= N - HALF)
    gy = np.where(natural, lanes, (lanes + KEPT) % N)
    cosine, sine = cos_sin(gy, grid)
    pick = natural[:, None]
    table = np.concatenate([np.where(pick, cosine, -sine), np.where(pick, sine, cosine)], axis=1)
    high, low = split(table)
    inverse_y = np.concatenate([high, high, low], axis=0)

    order = (first_gx[:, None] + np.arange(4)[None, :]).reshape(-1)
    cosine, sine = cos_sin(grid, order)
    cos_high, cos_low = split(cosine)
    sin_high, sin_low = split(sine)
    zero = np.zeros_like(cos_low)
    inverse_x = np.concatenate(
        [
            np.concatenate([cos_high, sin_high, cos_high, sin_high], axis=1),
            np.concatenate([cos_low, sin_low, zero, zero], axis=1),
        ],
        axis=0,
    )

    cosine, sine = cos_sin(order, grid)
    forward_x = stacked(cosine / N, sine / N)

    cosine, sine = cos_sin(grid, gy)
    pick = natural[None, :]
    table = np.concatenate([np.where(pick, cosine, -sine), np.where(pick, sine, cosine)], axis=0) / N
    forward_y = np.concatenate(split(table), axis=1)

    cosine, sine = cos_sin(kept, grid)
    forward_z = stacked(cosine / N, sine / N)
    return [inverse_z, inverse_y, inverse_x, forward_x, forward_y, forward_z]


def halves(value):
    high = value.astype(jnp.bfloat16)
    low = (value - high.astype(jnp.float32)).astype(jnp.bfloat16)
    return high, low


def dot(left, right):
    return jnp.dot(left, right, preferred_element_type=jnp.float32)


def kernel(
    wave,
    previous,
    potential,
    extent_hbm,
    metric_hbm,
    center,
    halfwidth,
    iz_hbm,
    iy_hbm,
    ix_hbm,
    fx_hbm,
    fy_hbm,
    fz_hbm,
    out,
    extent,
    metric,
    wbuf,
    pbuf,
    vbuf,
    iz,
    iy,
    ix,
    fx,
    fy,
    fz,
    vown,
    zboth,
    sbuf,
    rbuf,
    yre,
    yim,
    qhigh,
    qlow,
    gbuf,
    hbuf,
    base,
    wsem,
    psem,
    tsem,
    lsem,
    fsend,
    frecv,
    gsend,
    grecv,
    vsend,
    vrecv,
    esend,
    erecv,
    ready,
):
    me = lax.axis_index("fft")
    band = lax.axis_index("band")
    my_x, my_z = lax.div(band, 4), lax.rem(band, 4)
    my_y, my_low = lax.div(me, 4), lax.rem(me, 4)
    active = jnp.logical_or(me < ACTIVE // 2, me >= FFT - ACTIVE // 2)
    slot = jnp.where(me < ACTIVE // 2, me, me - (FFT - ACTIVE))
    lows = [my_low] + [lax.rem(my_low + i, 4) for i in (1, 2, 3)]
    rows_of_peers = [(lax.rem(my_y + dy, 8), lows) for dy in (4, 3, 5, 2, 6, 1, 7)] + [(my_y, lows[1:])]
    z_peers = [lax.rem(my_z + d, 4) for d in (2, 1, 3)]
    x_peers = [lax.rem(my_x + d, 4) for d in (2, 1, 3)]

    def hello(semaphore, where):
        pl.semaphore_signal(semaphore, inc=1, device_id=where, device_id_type=MESH)

    def wait_for(semaphore, count):
        @pl.when(count > 0)
        def _():
            pl.semaphore_wait(semaphore, count)

    def turn_of(y, place):
        usual = 4 * jnp.where(y <= 4, jnp.maximum(2 * y - 1, 0), 16 - 2 * y) + place
        return jnp.where(jnp.logical_and(band == 0, usual == 0), FFT, usual)

    my_turn = turn_of(my_y, my_low)
    earlier = jnp.where(band == 0, my_turn - 1, my_turn)
    z_shift = jnp.where(jnp.logical_and(me == 0, my_x == 0), 1, 0)
    x_shift = jnp.where(jnp.logical_and(me == 0, my_z == 0), 1, 0)

    def z_turn(z):
        return jnp.where(z < z_shift, 2, jnp.where(z < 3, z - z_shift, 3))

    def x_turn(x):
        return jnp.where(x < x_shift, 3, x - x_shift)

    my_z_turn, my_x_turn = z_turn(my_z), x_turn(my_x)

    def greet(semaphore, later):
        for y, places in rows_of_peers:
            for place in places:
                turn = turn_of(y, place)

                @pl.when(turn > my_turn if later else turn < my_turn)
                def _():
                    hello(semaphore, {"fft": y * 4 + place})

    barrier = pltpu.get_barrier_semaphore()
    greet(barrier, True)
    for z in z_peers:

        @pl.when(z_turn(z) > my_z_turn)
        def _():
            hello(barrier, {"band": my_x * 4 + z})

    for x in x_peers:

        @pl.when(x_turn(x) > my_x_turn)
        def _():
            hello(barrier, {"band": x * 4 + my_z})

    def wave_copies(b):
        return [
            pltpu.make_async_copy(
                wave.at[:, b, :, pl.ds(h * (N - HALF), HALF), :],
                wbuf.at[:, b, :, pl.ds(h * HALF, HALF), :],
                wsem.at[b, h],
            )
            for h in range(2)
        ]

    previous_copies = [
        pltpu.make_async_copy(
            previous.at[:, :, :, pl.ds(h * (N - HALF), HALF), :],
            pbuf.at[:, :, :, pl.ds(h * HALF, HALF), :],
            psem.at[h],
        )
        for h in range(2)
    ]
    small_refs = ((extent_hbm, extent), (metric_hbm, metric))
    load_v = pltpu.make_async_copy(potential, vown, lsem.at[0])
    small_copies = [pltpu.make_async_copy(a, b, lsem.at[i + 1]) for i, (a, b) in enumerate(small_refs)]
    table_refs = ((iz_hbm, iz), (iy_hbm, iy), (ix_hbm, ix), (fx_hbm, fx), (fy_hbm, fy), (fz_hbm, fz))
    table_copies = [pltpu.make_async_copy(a, b, tsem.at[i]) for i, (a, b) in enumerate(table_refs)]

    for copy in small_copies:
        copy.start()

    @pl.when(active)
    def _():
        for b in range(BANDS):
            for copy in wave_copies(b):
                copy.start()

    load_v.start()
    for copy in table_copies:
        copy.start()

    @pl.when(active)
    def _():
        for copy in previous_copies:
            copy.start()

    row = lax.broadcasted_iota(jnp.int32, (KEPT, N), 0)
    lane = lax.broadcasted_iota(jnp.int32, (KEPT, N), 1)
    natural = jnp.logical_or(lane < HALF, lane >= N - HALF)
    signed_gz = jnp.where(row < HALF, row, row - KEPT)
    place_gy = jnp.where(natural, lane, jnp.where(lane < KEPT, lane + KEPT, lane - KEPT))
    signed_gy = jnp.where(place_gy < N // 2, place_gy, place_gy - N)
    turn_sign = jnp.where(natural, -1.0, 1.0).astype(jnp.float32)

    def is_active(y):
        return jnp.logical_or(y < 2, y >= 6)

    def partner(y):
        return lax.rem(jnp.where(jnp.logical_or(y < 2, jnp.logical_or(y == 4, y == 5)), y + 2, y + 6), 8)

    def plane_of(y, place, c):
        if c < 4:
            return 4 * (y * 4 + place) + c
        return 4 * (partner(y) * 4 + place) + 3

    def keep_of(j):
        return (jnp.abs(signed_gz) <= extent[pl.ds(j, 1), :]).astype(jnp.float32)

    def both_parts(keep, real, imag):
        return keep * real + pltpu.roll(keep * imag, KEPT, axis=1)

    def to_planes():
        for b in range(BANDS):
            for copy in wave_copies(b):
                copy.wait()
        for j in range(4):
            keep = keep_of(j)
            for b in range(BANDS):
                packed = both_parts(keep, wbuf[0, b, j], wbuf[1, b, j])
                turned = pltpu.roll(packed, KEPT, axis=1) * turn_sign
                for t, part in enumerate((packed, turned)):
                    high, low = halves(part)
                    zboth[j, t * KEPT : (t + 1) * KEPT, b * N : (b + 1) * N] = high
                    zboth[j, N + t * KEPT : N + (t + 1) * KEPT, b * N : (b + 1) * N] = low
            both = dot(iz[...], zboth[j])
            both = both[:N] + both[N:]
            for b in range(BANDS):
                sbuf[pl.ds(2 * j + b, N, stride=8), :] = both[:, b * N : (b + 1) * N]
        for c in range(PLANES):
            mine = sbuf[pl.ds(pl.multiple_of(plane_of(my_y, my_low, c) * 8, 8), 8), :]
            rbuf[c, pl.ds(pl.multiple_of(slot * 8, 8), 8), :] = mine

    def scale():
        return jnp.full((1, N), 2.0, jnp.float32) / jnp.full((1, N), halfwidth[0], jnp.float32)

    def the_rest():
        for copy in previous_copies:
            copy.wait()
        step_z = (2.0 * math.pi / N) * signed_gz.astype(jnp.float32)
        step_y = (2.0 * math.pi / N) * signed_gy.astype(jnp.float32)
        plane_kinetic = metric[2] * (step_z * step_z) + metric[1] * (step_y * step_y)
        factor = scale()
        for j in range(4):
            gx = me * 4 + j
            signed_gx = jnp.where(gx < N // 2, gx, gx - N).astype(jnp.float32)
            step_x = (2.0 * math.pi / N) * signed_gx
            weight = factor * (0.5 * (metric[0] * (step_x * step_x) + plane_kinetic) - center[0])
            keep = keep_of(j)
            for b in range(BANDS):
                coefficient = both_parts(keep, wbuf[0, b, j], wbuf[1, b, j])
                base[b, j] = weight * coefficient - both_parts(keep, pbuf[0, b, j], pbuf[1, b, j])

    def send_planes(c):
        def send(y, places):
            for place in places:
                pltpu.make_async_remote_copy(
                    src_ref=sbuf.at[pl.ds(pl.multiple_of(plane_of(y, place, c) * 8, 8), 8), :],
                    dst_ref=rbuf.at[c, pl.ds(pl.multiple_of(slot * 8, 8), 8), :],
                    send_sem=fsend.at[c],
                    recv_sem=frecv.at[c],
                    device_id={"fft": y * 4 + place},
                    device_id_type=MESH,
                ).start()

        for y, places in rows_of_peers:
            if c < FEW:
                send(y, places)
            else:

                @pl.when(is_active(y))
                def _():
                    send(y, places)

    def send_columns(c):
        plane = plane_of(my_y, my_low, c)
        for y, places in rows_of_peers:

            @pl.when(is_active(y))
            def _():
                first = jnp.where(y < 2, y, y - 4) * 4
                for place in places:
                    pltpu.make_async_remote_copy(
                        src_ref=gbuf.at[c, pl.ds(pl.multiple_of((first + place) * 8, 8), 8), :],
                        dst_ref=hbuf.at[pl.ds(pl.multiple_of(plane * 8, 8), 8), :],
                        send_sem=gsend.at[c],
                        recv_sem=grecv.at[c],
                        device_id={"fft": y * 4 + place},
                        device_id_type=MESH,
                    ).start()

    def awaited(ref, send, recv):
        return pltpu.make_async_remote_copy(
            src_ref=ref, dst_ref=ref, send_sem=send, recv_sem=recv, device_id={"fft": me}, device_id_type=MESH
        )

    def send_v(where, phase, peer):
        pltpu.make_async_remote_copy(
            src_ref=where,
            dst_ref=where,
            send_sem=vsend.at[phase],
            recv_sem=vrecv.at[phase],
            device_id={"band": peer},
            device_id_type=MESH,
        ).start()

    my_rows = pl.ds(pl.multiple_of(band * 8, 8), 8)

    def send_v_along_z(z):
        @pl.when(active)
        def _():
            send_v(vbuf.at[pl.ds(0, 4), my_rows, :], PLANES, my_x * 4 + z)

        @pl.when(jnp.logical_not(active))
        def _():
            send_v(vbuf.at[pl.ds(0, FEW), my_rows, :], PLANES, my_x * 4 + z)

    def v_along_z(planes):
        return awaited(vbuf.at[pl.ds(0, planes), pl.ds(0, 24), :], vsend.at[PLANES], vrecv.at[PLANES])

    v_last_along_z = awaited(vbuf.at[4, pl.ds(0, 24), :], vsend.at[PLANES + 1], vrecv.at[PLANES + 1])

    def send_v_along_x(c):
        for x in x_peers:
            send_v(vbuf.at[c, pl.ds(pl.multiple_of(my_x * 32, 32), 32), :], c, x * 4 + my_z)

    def v_along_x(c):
        return awaited(vbuf.at[c, pl.ds(0, 96), :], vsend.at[c], vrecv.at[c])

    v_handed = pltpu.make_async_remote_copy(
        src_ref=vbuf.at[3, my_rows, :],
        dst_ref=vbuf.at[4, my_rows, :],
        send_sem=esend,
        recv_sem=erecv,
        device_id={"fft": partner(my_y) * 4 + my_low},
        device_id_type=MESH,
    )

    def work(c):
        high, low = halves(rbuf[c])
        plane = dot(jnp.concatenate([high, low, high], axis=1), iy[...])
        yre[...] = plane[:, :N]
        yim[...] = plane[:, N:]
        with jax.named_scope(f"wait_v{c}"):
            v_along_x(c).wait_recv()
        local_v = vbuf[c]
        for b in range(BANDS):
            rh, rl = halves(yre[pl.ds(b, KEPT, stride=2), :])
            ih, il = halves(yim[pl.ds(b, KEPT, stride=2), :])
            right = jnp.concatenate(
                [
                    jnp.concatenate([rh, ih], axis=1),
                    jnp.concatenate([-ih, rh], axis=1),
                    jnp.concatenate([rl, il], axis=1),
                    jnp.concatenate([-il, rl], axis=1),
                ],
                axis=0,
            )
            field = dot(ix[...], right)
            field = field[:N] + field[N:]
            rh, rl = halves(field[:, :N] * local_v)
            ih, il = halves(field[:, N:] * local_v)
            right = jnp.concatenate(
                [jnp.concatenate([rh, ih], axis=1), jnp.concatenate([rl, il], axis=1)], axis=0
            )
            both = dot(fx[...], right)
            both = both[:N] + both[N:]
            cos_part, sin_part = both[:KEPT], both[KEPT:]
            rows = slice(b * KEPT, (b + 1) * KEPT)
            high, low = halves(cos_part[:, :N] + sin_part[:, N:])
            qhigh[rows, :N] = high
            qlow[rows, :N] = low
            high, low = halves(cos_part[:, N:] - sin_part[:, :N])
            qhigh[rows, N:] = high
            qlow[rows, N:] = low
        wide = dot(qhigh[...], fy[...])
        packed = wide[:, :N] + wide[:, N:] + dot(qlow[...], fy[:, :N])
        for b in range(BANDS):
            gbuf[c, pl.ds(b, KEPT, stride=2), :] = packed[b * KEPT : (b + 1) * KEPT]
        with jax.named_scope(f"send_columns{c}"):
            send_columns(c)

        def keep_mine():
            mine = gbuf[c, pl.ds(pl.multiple_of(slot * 8, 8), 8), :]
            hbuf[pl.ds(pl.multiple_of(plane_of(my_y, my_low, c) * 8, 8), 8), :] = mine

        if c < FEW:
            pl.when(active)(keep_mine)
        else:
            keep_mine()

    with jax.named_scope("barrier"):
        wait_for(barrier, earlier + my_z_turn + my_x_turn)
        greet(ready.at[2], False)
        load_v.wait()
        for c in range(4):
            vbuf[c, my_rows, :] = vown[pl.ds(c, 8, stride=4), :]

    waits_for_first = jnp.logical_and(band == 0, me == 8)

    @pl.when(jnp.logical_not(jnp.logical_or(active, waits_for_first)))
    def _():
        v_handed.start()


    for z in z_peers:

        @pl.when(z_turn(z) < my_z_turn)
        def _():
            hello(ready.at[0], {"band": my_x * 4 + z})
            send_v_along_z(z)

    for x in x_peers:

        @pl.when(x_turn(x) < my_x_turn)
        def _():
            hello(ready.at[1], {"band": x * 4 + my_z})

    for copy in small_copies:
        copy.wait()
    table_copies[0].wait()

    @pl.when(active)
    def _():
        with jax.named_scope("planes"):
            to_planes()

    with jax.named_scope("wait_group"):
        wait_for(ready.at[2], FFT - 1 - earlier)

    @pl.when(waits_for_first)
    def _():
        v_handed.start()

    @pl.when(active)
    def _():
        with jax.named_scope("send"):
            for c in range(PLANES):
                send_planes(c)

    with jax.named_scope("wait_z"):
        wait_for(ready.at[0], 3 - my_z_turn)
    for z in z_peers:

        @pl.when(z_turn(z) > my_z_turn)
        def _():
            send_v_along_z(z)

    @pl.when(active)
    def _():
        with jax.named_scope("the_rest"):
            the_rest()

    with jax.named_scope("wait_vz"):

        @pl.when(active)
        def _():
            v_handed.wait_recv()
            for z in z_peers:
                send_v(vbuf.at[4, my_rows, :], PLANES + 1, my_x * 4 + z)
            v_along_z(4).wait_recv()

        @pl.when(jnp.logical_not(active))
        def _():
            v_along_z(FEW).wait_recv()

        wait_for(ready.at[1], 3 - my_x_turn)

    for c in range(FEW):
        send_v_along_x(c)

    @pl.when(active)
    def _():
        send_v_along_x(3)
        with jax.named_scope("wait_vlast"):
            v_last_along_z.wait_recv()
        send_v_along_x(4)

    for copy in table_copies[1:]:
        copy.wait()

    for c in range(FEW):
        with jax.named_scope(f"wait_planes{c}"):

            @pl.when(active)
            def _():
                awaited(rbuf.at[c, pl.ds(0, 8 * (ACTIVE - 1)), :], fsend.at[c], frecv.at[c]).wait_recv()

            @pl.when(jnp.logical_not(active))
            def _():
                awaited(rbuf.at[c], fsend.at[c], frecv.at[c]).wait_recv()

        work(c)

    def peers_with(c):
        return FFT - 1 if c < FEW else ACTIVE - 1

    @pl.when(active)
    def _():
        for c in range(FEW, PLANES):
            with jax.named_scope(f"wait_planes{c}"):
                awaited(rbuf.at[c, pl.ds(0, 8 * (ACTIVE - 1)), :], fsend.at[c], frecv.at[c]).wait_recv()
            work(c)
        factor = scale()
        for c in range(PLANES):
            with jax.named_scope(f"wait_columns{c}"):
                awaited(hbuf.at[pl.ds(0, 8 * peers_with(c)), :], gsend.at[c], grecv.at[c]).wait_recv()
        for j in range(4):
            h0, l0 = halves(hbuf[pl.ds(2 * j, N, stride=8), :])
            h1, l1 = halves(hbuf[pl.ds(2 * j + 1, N, stride=8), :])
            right = jnp.concatenate(
                [jnp.concatenate([h0, h1], axis=1), jnp.concatenate([l0, l1], axis=1)], axis=0
            )
            both = dot(fz[...], right)
            both = both[:N] + both[N:]
            keep = keep_of(j)
            keep = keep + pltpu.roll(keep, KEPT, axis=1)
            for b in range(BANDS):
                cos_part = both[:KEPT, b * N : (b + 1) * N]
                sin_part = both[KEPT:, b * N : (b + 1) * N]
                applied = cos_part - turn_sign * pltpu.roll(sin_part, KEPT, axis=1)
                out[b, j] = keep * (factor * applied) + base[b, j]

    with jax.named_scope("wait_sends"):

        @pl.when(active)
        def _():
            v_along_z(4).wait_send()
            v_last_along_z.wait_send()
            for c in range(FEW, PLANES):
                v_along_x(c).wait_send()
            for c in range(PLANES):
                awaited(sbuf.at[pl.ds(0, 8 * peers_with(c)), :], fsend.at[c], frecv.at[c]).wait_send()
                awaited(gbuf.at[c, pl.ds(0, 8 * (ACTIVE - 1)), :], gsend.at[c], grecv.at[c]).wait_send()

        @pl.when(jnp.logical_not(active))
        def _():
            v_handed.wait_send()
            v_along_z(FEW).wait_send()
            for c in range(FEW):
                awaited(gbuf.at[c], gsend.at[c], grecv.at[c]).wait_send()

        for c in range(FEW):
            v_along_x(c).wait_send()


def expand(packed, out, obuf, sem):
    me = lax.axis_index("fft")
    active = jnp.logical_or(me < ACTIVE // 2, me >= FFT - ACTIVE // 2)
    lane = lax.broadcasted_iota(jnp.int32, (KEPT, N), 1)
    natural = jnp.logical_or(lane < HALF, lane >= N - HALF)
    copies = [pltpu.make_async_copy(obuf.at[:, b], out.at[:, b], sem.at[b]) for b in range(BANDS)]

    @pl.when(active)
    def _():
        for b in range(BANDS):
            for j in range(4):
                both = packed[b, j]
                for t, part in enumerate((both, pltpu.roll(both, KEPT, axis=1))):
                    part = jnp.where(natural, part, 0.0)
                    obuf[t, b, j, :HALF, :] = part[:HALF]
                    obuf[t, b, j, HALF : N - HALF, :] = jnp.zeros((KEPT, N), jnp.float32)
                    obuf[t, b, j, N - HALF :, :] = part[HALF:]
            copies[b].start()

    @pl.when(jnp.logical_not(active))
    def _():
        obuf[...] = jnp.zeros_like(obuf)
        for copy in copies:
            copy.start()

    for copy in copies:
        copy.wait()


def local(tables, wave, previous, potential, column_extent, metric, center, halfwidth):
    any_spec = pl.BlockSpec(memory_space=pltpu.HBM)
    vmem_spec = pl.BlockSpec(memory_space=pltpu.VMEM)
    smem_spec = pl.BlockSpec(memory_space=pltpu.SMEM)
    f32, bf16 = jnp.float32, jnp.bfloat16
    dma = pltpu.SemaphoreType.DMA
    packed = pl.pallas_call(
        kernel,
        out_shape=pltpu.VMEM((BANDS, 4, KEPT, N), f32),
        in_specs=[any_spec] * 5 + [smem_spec] * 2 + [any_spec] * 6,
        out_specs=vmem_spec,
        scratch_shapes=[
            pltpu.VMEM((4, N), jnp.int32),
            pltpu.SMEM((3,), f32),
            pltpu.VMEM((2, BANDS, 4, KEPT, N), f32),
            pltpu.VMEM((2, BANDS, 4, KEPT, N), f32),
            pltpu.VMEM((PLANES, N, N), f32),
            *[pltpu.VMEM(table.shape, bf16) for table in tables],
            pltpu.VMEM((32, N), f32),
            pltpu.VMEM((4, 2 * N, 2 * N), bf16),
            pltpu.VMEM((8 * N, N), f32),
            pltpu.VMEM((PLANES, N, N), f32),
            pltpu.VMEM((N, N), f32),
            pltpu.VMEM((N, N), f32),
            pltpu.VMEM((N, 2 * N), bf16),
            pltpu.VMEM((N, 2 * N), bf16),
            pltpu.VMEM((PLANES, N, N), f32),
            pltpu.VMEM((8 * N, N), f32),
            pltpu.VMEM((BANDS, 4, KEPT, N), f32),
            dma((BANDS, 2)),
            dma((2,)),
            dma((6,)),
            dma((3,)),
            dma((PLANES,)),
            dma((PLANES,)),
            dma((PLANES,)),
            dma((PLANES,)),
            dma((PLANES + 2,)),
            dma((PLANES + 2,)),
            dma,
            dma,
            pltpu.SemaphoreType.REGULAR((3,)),
        ],
        compiler_params=pltpu.CompilerParams(
            collective_id=0, has_side_effects=True, vmem_limit_bytes=24 * 1024 * 1024
        ),
    )(
        *[
            pltpu.with_memory_space_constraint(value, pltpu.HBM)
            for value in (wave, previous, potential.reshape(32, N), column_extent, metric)
        ],
        center,
        halfwidth,
        *[pltpu.with_memory_space_constraint(table, pltpu.HBM) for table in tables],
    )
    return pl.pallas_call(
        expand,
        out_shape=jax.ShapeDtypeStruct(wave.shape, f32),
        in_specs=[vmem_spec],
        out_specs=any_spec,
        scratch_shapes=[pltpu.VMEM((2, BANDS, 4, N, N), f32), dma((BANDS,))],
        compiler_params=pltpu.CompilerParams(vmem_limit_bytes=8 * 1024 * 1024),
    )(packed)


def solution(mesh):
    tables = [jnp.asarray(table) for table in make_tables()]
    in_specs = (
        P(None, "band", "fft", None, None),
        P(None, "band", "fft", None, None),
        P("band", "fft", None),
        P("fft", None),
        P(),
        P(),
        P(),
    )
    out_specs = P(None, "band", "fft", None, None)
    return jax.shard_map(
        functools.partial(local, tables), mesh=mesh, in_specs=in_specs, out_specs=out_specs, check_vma=False
    )
```

```python
import functools
import math

import jax
import jax.numpy as jnp
import numpy as np
from jax import lax
from jax.experimental import pallas as pl
from jax.experimental.pallas import tpu as pltpu
from jax.sharding import PartitionSpec as P

N = 128
KEPT = 64
HALF = KEPT // 2
FFT = 32
ACTIVE = 16
BANDS = 2
PLANES = 5
FEW = 3
MESH = pl.DeviceIdType.MESH


def kept_indices():
    return np.concatenate([np.arange(HALF), np.arange(N - HALF, N)])


def cos_sin(rows, cols):
    angles = (np.outer(rows, cols) % N) * (2.0 * math.pi / N)
    return np.cos(angles), np.sin(angles)


def split(table):
    high = table.astype(jnp.bfloat16)
    low = (table - high.astype(np.float64)).astype(jnp.bfloat16)
    return high, low


def stacked(cosine, sine):
    cos_high, cos_low = split(cosine)
    sin_high, sin_low = split(sine)
    zero = np.zeros_like(cos_low)
    return np.concatenate(
        [
            np.concatenate([cos_high, cos_high], axis=1),
            np.concatenate([sin_high, sin_high], axis=1),
            np.concatenate([cos_low, zero], axis=1),
            np.concatenate([sin_low, zero], axis=1),
        ],
        axis=0,
    )


def make_tables():
    grid = np.arange(N)
    kept = kept_indices()
    slots = np.arange(ACTIVE)
    first_gx = 4 * np.where(slots < ACTIVE // 2, slots, slots + FFT - ACTIVE)

    cosine, sine = cos_sin(grid, kept)
    high, low = split(np.concatenate([cosine, sine], axis=1))
    zero = np.zeros_like(low)
    inverse_z = np.concatenate([np.concatenate([high, high], axis=1), np.concatenate([low, zero], axis=1)], axis=0)

    lanes = np.arange(N)
    natural = (lanes < HALF) | (lanes >= N - HALF)
    gy = np.where(natural, lanes, (lanes + KEPT) % N)
    cosine, sine = cos_sin(gy, grid)
    pick = natural[:, None]
    table = np.concatenate([np.where(pick, cosine, -sine), np.where(pick, sine, cosine)], axis=1)
    high, low = split(table)
    inverse_y = np.concatenate([high, high, low], axis=0)

    order = (first_gx[:, None] + np.arange(4)[None, :]).reshape(-1)
    cosine, sine = cos_sin(grid, order)
    cos_high, cos_low = split(cosine)
    sin_high, sin_low = split(sine)
    zero = np.zeros_like(cos_low)
    inverse_x = np.concatenate(
        [
            np.concatenate([cos_high, sin_high, cos_high, sin_high], axis=1),
            np.concatenate([cos_low, sin_low, zero, zero], axis=1),
        ],
        axis=0,
    )

    cosine, sine = cos_sin(order, grid)
    forward_x = stacked(cosine / N, sine / N)

    cosine, sine = cos_sin(grid, gy)
    pick = natural[None, :]
    table = np.concatenate([np.where(pick, cosine, -sine), np.where(pick, sine, cosine)], axis=0) / N
    forward_y = np.concatenate(split(table), axis=1)

    cosine, sine = cos_sin(kept, grid)
    forward_z = stacked(cosine / N, sine / N)
    return [inverse_z, inverse_y, inverse_x, forward_x, forward_y, forward_z]


def halves(value):
    high = value.astype(jnp.bfloat16)
    low = (value - high.astype(jnp.float32)).astype(jnp.bfloat16)
    return high, low


def dot(left, right):
    return jnp.dot(left, right, preferred_element_type=jnp.float32)


def kernel(
    wave,
    previous,
    potential,
    extent_hbm,
    metric_hbm,
    center,
    halfwidth,
    iz_hbm,
    iy_hbm,
    ix_hbm,
    fx_hbm,
    fy_hbm,
    fz_hbm,
    out,
    extent,
    metric,
    wbuf,
    pbuf,
    vbuf,
    iz,
    iy,
    ix,
    fx,
    fy,
    fz,
    vown,
    zboth,
    sbuf,
    rbuf,
    yre,
    yim,
    fbuf,
    qhigh,
    qlow,
    gbuf,
    hbuf,
    base,
    wsem,
    psem,
    tsem,
    lsem,
    fsend,
    frecv,
    gsend,
    grecv,
    vsend,
    vrecv,
    esend,
    erecv,
    ready,
):
    me = lax.axis_index("fft")
    band = lax.axis_index("band")
    my_x, my_z = lax.div(band, 4), lax.rem(band, 4)
    my_y, my_low = lax.div(me, 4), lax.rem(me, 4)
    active = jnp.logical_or(me < ACTIVE // 2, me >= FFT - ACTIVE // 2)
    slot = jnp.where(me < ACTIVE // 2, me, me - (FFT - ACTIVE))
    lows = [my_low] + [lax.rem(my_low + i, 4) for i in (1, 2, 3)]
    rows_of_peers = [(lax.rem(my_y + dy, 8), lows) for dy in (4, 3, 5, 2, 6, 1, 7)] + [(my_y, lows[1:])]
    z_peers = [lax.rem(my_z + d, 4) for d in (2, 1, 3)]
    x_peers = [lax.rem(my_x + d, 4) for d in (2, 1, 3)]

    def hello(semaphore, where):
        pl.semaphore_signal(semaphore, inc=1, device_id=where, device_id_type=MESH)

    def wait_for(semaphore, count):
        @pl.when(count > 0)
        def _():
            pl.semaphore_wait(semaphore, count)

    def turn_of(y, place):
        usual = 4 * jnp.where(y < 4, y, 11 - y) + place
        return jnp.where(jnp.logical_and(band == 0, usual == 0), FFT, usual)

    my_turn = turn_of(my_y, my_low)
    earlier = jnp.where(band == 0, my_turn - 1, my_turn)
    z_shift = jnp.where(jnp.logical_and(me == 0, my_x == 0), 1, 0)
    x_shift = jnp.where(jnp.logical_and(me == 0, my_z == 0), 1, 0)

    def z_turn(z):
        return jnp.where(z < z_shift, 1, jnp.where(z == 1, 1 - z_shift, z))

    def x_turn(x):
        return jnp.where(x < x_shift, 3, x - x_shift)

    my_z_turn, my_x_turn = z_turn(my_z), x_turn(my_x)

    late = jnp.logical_and(band == 0, me == 0)
    side_2 = jnp.logical_and(my_y >= 2, my_y < 4)
    side_6 = my_y >= 6

    my_row = jnp.where(my_y < 4, my_y, 11 - my_y)
    y_order = (4, 5, 6, 3, 7, 2, 1, 0)

    def greet(semaphore, later):
        def to(y, line, core):
            place = 2 * line + core
            if y == 0 and core == 0 and not later:

                @pl.when(jnp.logical_or(band != 0, line != 0))
                def _():
                    hello(semaphore, {"fft": y * 4 + place})
            else:
                hello(semaphore, {"fft": y * 4 + place})

        for y in y_order:
            y_row = y if y < 4 else 11 - y
            near = y_row > my_row if later else y_row < my_row
            if later and y >= 6:
                near = near & jnp.logical_not(side_2)
            if not later and 2 <= y < 4:
                near = near & jnp.logical_not(side_6)

            @pl.when(near)
            def _():
                for line in range(2):
                    for core in range(2):
                        to(y, line, core)

        for place in range(4):

            @pl.when(place > my_low if later else place < my_low)
            def _():
                if place > 0:
                    hello(semaphore, {"fft": my_y * 4 + place})
                else:

                    @pl.when(jnp.logical_or(band != 0, my_y > 0))
                    def _():
                        hello(semaphore, {"fft": my_y * 4})

    def greet_all(semaphore):
        for y in range(FFT // 4):
            for place in range(4):
                if y + place > 0:
                    hello(semaphore, {"fft": y * 4 + place})

    def is_late_row(y):
        return jnp.logical_and(band == 0, y == 0)

    load_v = pltpu.make_async_copy(potential, vown, lsem.at[0])
    load_v.start()
    barrier = pltpu.get_barrier_semaphore()
    direct = jnp.logical_not(active)
    early = jnp.logical_and(direct, my_z < 2)
    tardy = jnp.logical_and(direct, my_z >= 2)

    @pl.when(jnp.logical_not(late))
    def _():
        greet(barrier, True)

    @pl.when(jnp.logical_and(band == 0, me > 0))
    def _():
        hello(barrier, {"fft": 0})

    @pl.when(my_z < 2)
    def _():
        for z in (2, 3):
            for x in x_peers:
                hello(barrier, {"band": x * 4 + z})

    for z in z_peers:

        @pl.when(z_turn(z) > my_z_turn)
        def _():
            hello(barrier, {"band": my_x * 4 + z})

    for x in x_peers:

        @pl.when(x_turn(x) > my_x_turn)
        def _():
            hello(barrier, {"band": x * 4 + my_z})

    def wave_copies(b):
        return [
            pltpu.make_async_copy(
                wave.at[:, b, :, pl.ds(h * (N - HALF), HALF), :],
                wbuf.at[:, b, :, pl.ds(h * HALF, HALF), :],
                wsem.at[b, h],
            )
            for h in range(2)
        ]

    previous_copies = [
        pltpu.make_async_copy(
            previous.at[:, :, :, pl.ds(h * (N - HALF), HALF), :],
            pbuf.at[:, :, :, pl.ds(h * HALF, HALF), :],
            psem.at[h],
        )
        for h in range(2)
    ]
    small_refs = ((extent_hbm, extent), (metric_hbm, metric))
    small_copies = [pltpu.make_async_copy(a, b, lsem.at[i + 1]) for i, (a, b) in enumerate(small_refs)]
    table_refs = ((iz_hbm, iz), (iy_hbm, iy), (ix_hbm, ix), (fx_hbm, fx), (fy_hbm, fy), (fz_hbm, fz))
    table_copies = [pltpu.make_async_copy(a, b, tsem.at[i]) for i, (a, b) in enumerate(table_refs)]

    for copy in small_copies:
        copy.start()

    @pl.when(active)
    def _():
        for b in range(BANDS):
            for copy in wave_copies(b):
                copy.start()

    for copy in table_copies:
        copy.start()

    @pl.when(active)
    def _():
        for copy in previous_copies:
            copy.start()

    row = lax.broadcasted_iota(jnp.int32, (KEPT, N), 0)
    lane = lax.broadcasted_iota(jnp.int32, (KEPT, N), 1)
    natural = jnp.logical_or(lane < HALF, lane >= N - HALF)
    signed_gz = jnp.where(row < HALF, row, row - KEPT)
    place_gy = jnp.where(natural, lane, jnp.where(lane < KEPT, lane + KEPT, lane - KEPT))
    signed_gy = jnp.where(place_gy < N // 2, place_gy, place_gy - N)
    turn_sign = jnp.where(natural, -1.0, 1.0).astype(jnp.float32)

    def is_active(y):
        return jnp.logical_or(y < 2, y >= 6)

    def partner(y):
        return lax.rem(jnp.where(jnp.logical_or(y < 2, jnp.logical_or(y == 4, y == 5)), y + 2, y + 6), 8)

    def plane_of(y, place, c):
        if c < 4:
            return 4 * (y * 4 + place) + c
        if isinstance(y, int):
            return 4 * ((y + 2 if y < 2 else y - 2) * 4 + place) + 3
        return 4 * (partner(y) * 4 + place) + 3

    def keep_of(j):
        return (jnp.abs(signed_gz) <= extent[pl.ds(j, 1), :]).astype(jnp.float32)

    def both_parts(keep, real, imag):
        return keep * real + pltpu.roll(keep * imag, KEPT, axis=1)

    def to_planes():
        for b in range(BANDS):
            for copy in wave_copies(b):
                copy.wait()
        for j in range(4):
            keep = keep_of(j)
            for b in range(BANDS):
                packed = both_parts(keep, wbuf[0, b, j], wbuf[1, b, j])
                turned = pltpu.roll(packed, KEPT, axis=1) * turn_sign
                for t, part in enumerate((packed, turned)):
                    high, low = halves(part)
                    zboth[j, t * KEPT : (t + 1) * KEPT, b * N : (b + 1) * N] = high
                    zboth[j, N + t * KEPT : N + (t + 1) * KEPT, b * N : (b + 1) * N] = low
            both = dot(iz[...], zboth[j])
            both = both[:N] + both[N:]
            for b in range(BANDS):
                sbuf[pl.ds(2 * j + b, N, stride=8), :] = both[:, b * N : (b + 1) * N]
        for c in range(PLANES):
            mine = sbuf[pl.ds(pl.multiple_of(plane_of(my_y, my_low, c) * 8, 8), 8), :]
            rbuf[c, pl.ds(pl.multiple_of(slot * 8, 8), 8), :] = mine

    def scale():
        return jnp.full((1, N), 2.0, jnp.float32) / jnp.full((1, N), halfwidth[0], jnp.float32)

    def the_rest():
        for copy in previous_copies:
            copy.wait()
        step_z = (2.0 * math.pi / N) * signed_gz.astype(jnp.float32)
        step_y = (2.0 * math.pi / N) * signed_gy.astype(jnp.float32)
        plane_kinetic = metric[2] * (step_z * step_z) + metric[1] * (step_y * step_y)
        factor = scale()
        for j in range(4):
            gx = me * 4 + j
            signed_gx = jnp.where(gx < N // 2, gx, gx - N).astype(jnp.float32)
            step_x = (2.0 * math.pi / N) * signed_gx
            weight = factor * (0.5 * (metric[0] * (step_x * step_x) + plane_kinetic) - center[0])
            keep = keep_of(j)
            for b in range(BANDS):
                coefficient = both_parts(keep, wbuf[0, b, j], wbuf[1, b, j])
                base[b, j] = weight * coefficient - both_parts(keep, pbuf[0, b, j], pbuf[1, b, j])

    def send_plane(c, y, place):
        pltpu.make_async_remote_copy(
            src_ref=sbuf.at[pl.ds(pl.multiple_of(plane_of(y, place, c) * 8, 8), 8), :],
            dst_ref=rbuf.at[c, pl.ds(pl.multiple_of(slot * 8, 8), 8), :],
            send_sem=fsend.at[c],
            recv_sem=frecv.at[c],
            device_id={"fft": y * 4 + place},
            device_id_type=MESH,
        ).start()

    def to_others(y, send):
        @pl.when(my_y == y)
        def _():
            for place in lows[1:]:
                send(y, place)

        @pl.when(my_y != y)
        def _():
            for place in lows:
                send(y, place)

    def send_planes(c, order):
        def send(y, place):
            send_plane(c, y, place)

        def unless_late(y, place):
            @pl.when(jnp.logical_and(place > 0, y * 4 + place != me))
            def _():
                send(y, place)

        for y in order:
            if 2 <= y < 6:
                if c < FEW:
                    for place in lows:
                        send(y, place)
            elif y > 0:
                to_others(y, send)
            else:

                @pl.when(band == 0)
                def _():
                    for place in lows:
                        unless_late(0, place)

                @pl.when(band != 0)
                def _():
                    to_others(0, send)

    def send_columns(c):
        plane = plane_of(my_y, my_low, c)

        def send(y, place):
            first = (y if y < 2 else y - 4) * 4
            pltpu.make_async_remote_copy(
                src_ref=gbuf.at[c, pl.ds(pl.multiple_of((first + place) * 8, 8), 8), :],
                dst_ref=hbuf.at[pl.ds(pl.multiple_of(plane * 8, 8), 8), :],
                send_sem=gsend.at[c],
                recv_sem=grecv.at[c],
                device_id={"fft": y * 4 + place},
                device_id_type=MESH,
            ).start()

        @pl.when(active)
        def _():
            for y in (7, 0, 6, 1):
                to_others(y, send)

        if c < FEW:

            @pl.when(jnp.logical_not(active))
            def _():
                for y in (7, 0, 6, 1):
                    for place in lows:
                        send(y, place)

    def awaited(ref, send, recv):
        return pltpu.make_async_remote_copy(
            src_ref=ref, dst_ref=ref, send_sem=send, recv_sem=recv, device_id={"fft": me}, device_id_type=MESH
        )

    def send_v(where, phase, peer):
        pltpu.make_async_remote_copy(
            src_ref=where,
            dst_ref=where,
            send_sem=vsend.at[phase],
            recv_sem=vrecv.at[phase],
            device_id={"band": peer},
            device_id_type=MESH,
        ).start()

    my_rows = pl.ds(pl.multiple_of(band * 8, 8), 8)

    def v_part(planes, rows):
        return vbuf.at[pl.ds(0, planes), rows, :]

    def v_rows(z):
        return pl.ds(pl.multiple_of(my_x * 32 + z * 8, 8), 8)

    def for_kind(function):
        pl.when(active)(lambda: function(4))
        pl.when(jnp.logical_not(active))(lambda: function(FEW))

    def takes_z(z):
        return jnp.logical_not(jnp.logical_and(tardy, z < 2))

    def send_v_along_z(z, turn):
        @pl.when(takes_z(z))
        def _():
            for_kind(lambda planes: send_v(v_part(planes, my_rows), turn, my_x * 4 + z))

    def v_along_z(planes, turn):
        return awaited(v_part(planes, pl.ds(0, 8)), vsend.at[turn], vrecv.at[turn])

    def send_v_along_x(z):
        for x in x_peers:
            for_kind(lambda planes: send_v(v_part(planes, v_rows(z)), 4, x * 4 + my_z))

    def send_v_directly(part, phase):
        for z in range(2):
            for x in x_peers + [my_x]:
                send_v(part, phase, x * 4 + z)

    def v_wait(planes, phase, rows):
        return awaited(v_part(planes, pl.ds(0, rows)), vsend.at[phase], vrecv.at[phase])

    def v_last(phase, rows):
        return awaited(vbuf.at[4, pl.ds(0, rows), :], vsend.at[phase], vrecv.at[phase])

    v_handed = pltpu.make_async_remote_copy(
        src_ref=vbuf.at[3, my_rows, :],
        dst_ref=vbuf.at[4, my_rows, :],
        send_sem=esend,
        recv_sem=erecv,
        device_id={"fft": partner(my_y) * 4 + my_low},
        device_id_type=MESH,
    )

    def field(c):
        with jax.named_scope(f"wait_planes{c}"):

            @pl.when(active)
            def _():
                awaited(rbuf.at[c, pl.ds(0, 8 * (ACTIVE - 1)), :], fsend.at[c], frecv.at[c]).wait_recv()

            if c < FEW:

                @pl.when(jnp.logical_not(active))
                def _():
                    awaited(rbuf.at[c], fsend.at[c], frecv.at[c]).wait_recv()

        high, low = halves(rbuf[c])
        plane = dot(jnp.concatenate([high, low, high], axis=1), iy[...])
        yre[...] = plane[:, :N]
        yim[...] = plane[:, N:]
        for b in range(BANDS):
            rh, rl = halves(yre[pl.ds(b, KEPT, stride=2), :])
            ih, il = halves(yim[pl.ds(b, KEPT, stride=2), :])
            right = jnp.concatenate(
                [
                    jnp.concatenate([rh, ih], axis=1),
                    jnp.concatenate([-ih, rh], axis=1),
                    jnp.concatenate([rl, il], axis=1),
                    jnp.concatenate([-il, rl], axis=1),
                ],
                axis=0,
            )
            both = dot(ix[...], right)
            fbuf[c, b] = both[:N] + both[N:]

    def back(c):
        if c == 0:
            with jax.named_scope("wait_v"):

                def arrived(planes):
                    @pl.when(early)
                    def _():
                        v_wait(planes, 4, 48).wait_recv()
                        v_wait(planes, 7, 64).wait_recv()

                    @pl.when(jnp.logical_not(early))
                    def _():
                        v_wait(planes, 4, 96).wait_recv()

                for_kind(arrived)
        if c == 4:
            with jax.named_scope("wait_v4"):


                @pl.when(my_z < 2)
                def _():
                    v_last(6, 48).wait_recv()
                    v_last(8, 64).wait_recv()

                @pl.when(my_z >= 2)
                def _():
                    v_last(6, 96).wait_recv()

        local_v = vbuf[c]
        for b in range(BANDS):
            rh, rl = halves(fbuf[c, b, :, :N] * local_v)
            ih, il = halves(fbuf[c, b, :, N:] * local_v)
            right = jnp.concatenate(
                [jnp.concatenate([rh, ih], axis=1), jnp.concatenate([rl, il], axis=1)], axis=0
            )
            both = dot(fx[...], right)
            both = both[:N] + both[N:]
            cos_part, sin_part = both[:KEPT], both[KEPT:]
            rows = slice(b * KEPT, (b + 1) * KEPT)
            high, low = halves(cos_part[:, :N] + sin_part[:, N:])
            qhigh[rows, :N] = high
            qlow[rows, :N] = low
            high, low = halves(cos_part[:, N:] - sin_part[:, :N])
            qhigh[rows, N:] = high
            qlow[rows, N:] = low
        wide = dot(qhigh[...], fy[...])
        packed = wide[:, :N] + wide[:, N:] + dot(qlow[...], fy[:, :N])
        for b in range(BANDS):
            gbuf[c, pl.ds(b, KEPT, stride=2), :] = packed[b * KEPT : (b + 1) * KEPT]
        with jax.named_scope(f"send_columns{c}"):
            send_columns(c)

        def keep_mine():
            mine = gbuf[c, pl.ds(pl.multiple_of(slot * 8, 8), 8), :]
            hbuf[pl.ds(pl.multiple_of(plane_of(my_y, my_low, c) * 8, 8), 8), :] = mine

        if c < FEW:
            pl.when(active)(keep_mine)
        else:
            keep_mine()

    with jax.named_scope("barrier"):
        wait_for(barrier, earlier + my_z_turn + my_x_turn + jnp.where(my_z >= 2, 6, 0) - jnp.where(side_6, 8, 0))
        load_v.wait()
        for c in range(4):
            vbuf[c, my_rows, :] = vown[pl.ds(c, 8, stride=4), :]

    @pl.when(tardy)
    def _():
        send_v_directly(v_part(FEW, my_rows), 7)

    @pl.when(late)
    def _():
        greet_all(ready.at[3])

    @pl.when(jnp.logical_not(late))
    def _():
        greet(ready.at[2], False)

    waits_for_first = jnp.logical_and(band == 0, me == 8)

    @pl.when(jnp.logical_not(jnp.logical_or(active, waits_for_first)))
    def _():
        v_handed.start()


    for z in z_peers:

        @pl.when(z_turn(z) < my_z_turn)
        def _():
            hello(ready.at[0], {"band": my_x * 4 + z})
            send_v_along_z(z, my_z_turn)

    for x in x_peers:

        @pl.when(x_turn(x) < my_x_turn)
        def _():
            hello(ready.at[1], {"band": x * 4 + my_z})

    for copy in small_copies:
        copy.wait()
    table_copies[0].wait()

    @pl.when(active)
    def _():
        with jax.named_scope("planes"):
            to_planes()

    def hand_on(z, later):
        @pl.when(active & (z_turn(z) > my_z_turn if later else z_turn(z) < my_z_turn) & jnp.logical_not((my_z >= 2) & (z < 2)))
        def _():
            send_v(vbuf.at[4, my_rows, :], 5, my_x * 4 + z)

    @pl.when(jnp.logical_and(active, jnp.logical_not(late)))
    def _():
        with jax.named_scope("wait_handed"):
            v_handed.wait_recv()
        for z in z_peers:
            hand_on(z, False)

        @pl.when(my_z >= 2)
        def _():
            send_v_directly(vbuf.at[4, my_rows, :], 8)

    with jax.named_scope("wait_group"):
        wait_for(
            ready.at[2],
            jnp.where(late, 0, jnp.where(band == 0, FFT - 2, FFT - 1) - earlier - jnp.where(side_2, 8, 0)),
        )


    @pl.when(my_y == 1)
    def _():
        for y in (7, 6):
            hello(ready.at[4], {"fft": y * 4 + my_low})

    with jax.named_scope("send"):

        @pl.when(my_y < 2)
        def _():
            for c in range(PLANES):
                send_planes(c, (4, 3, 5, 2, 6, 7, 1, 0))

        @pl.when(side_6)
        def _():
            for c in range(2):
                send_planes(c, (4, 5, 1, 0, 6, 7))
            pl.semaphore_wait(ready.at[4], 1)
            for c in range(2):
                send_planes(c, (3, 2))
            for c in range(2, PLANES):
                send_planes(c, (3, 4, 2, 5, 1, 0, 6, 7))

    with jax.named_scope("wait_z"):
        wait_for(ready.at[0], 3 - my_z_turn)

    @pl.when(jnp.logical_not(late))
    def _():
        for z in z_peers:
            hand_on(z, True)

    for z in z_peers:

        @pl.when(z_turn(z) > my_z_turn)
        def _():
            send_v_along_z(z, my_z_turn)

    with jax.named_scope("wait_x"):
        wait_for(ready.at[1], 3 - my_x_turn)
    send_v_along_x(my_z)

    @pl.when(active)
    def _():
        with jax.named_scope("the_rest"):
            the_rest()

    def forward_v(turn, z):
        @pl.when(turn != my_z_turn if turn < 2 else jnp.logical_and(turn != my_z_turn, jnp.logical_not(early)))
        def _():
            with jax.named_scope(f"wait_vz{turn}"):
                for_kind(lambda planes: v_along_z(planes, turn).wait_recv())
            send_v_along_x(z)

    def z_of(turn):
        return jnp.abs(turn - z_shift) if turn < 2 else turn

    for turn in range(2):
        forward_v(turn, z_of(turn))

    @pl.when(jnp.logical_and(band == 0, me > 0))
    def _():
        with jax.named_scope("wait_late"):
            pl.semaphore_wait(ready.at[3], 1)

        @pl.when(me == 8)
        def _():
            v_handed.start()

        @pl.when(active)
        def _():
            for c in range(PLANES):
                send_plane(c, 0, 0)

    forward_v(2, z_of(2))

    forward_v(3, z_of(3))

    @pl.when(late)
    def _():
        v_handed.wait_recv()
        for z in z_peers:
            hand_on(z, False)
            hand_on(z, True)

    for copy in table_copies[1:]:
        copy.wait()

    def forward_last():
        with jax.named_scope("wait_vlast"):

            def forward(blocks):
                v_last(5, 8 * blocks - 8 if blocks > 2 else 8).wait_recv()
                for x in x_peers:
                    send_v(vbuf.at[4, pl.ds(pl.multiple_of(my_x * 32, 32), 8 * blocks), :], 6, x * 4 + my_z)

            pl.when(my_z < 2)(lambda: forward(2))
            pl.when(my_z >= 2)(lambda: forward(4))

    for c in range(FEW):
        field(c)
        back(c)
        if c == 0:
            pl.when(active)(forward_last)

    def peers_with(c):
        return FFT - 1 if c < FEW else ACTIVE - 1

    @pl.when(active)
    def _():
        for c in range(FEW, PLANES):
            field(c)
            back(c)
        factor = scale()
        for c in range(PLANES):
            with jax.named_scope(f"wait_columns{c}"):
                awaited(hbuf.at[pl.ds(0, 8 * peers_with(c)), :], gsend.at[c], grecv.at[c]).wait_recv()
        for j in range(4):
            h0, l0 = halves(hbuf[pl.ds(2 * j, N, stride=8), :])
            h1, l1 = halves(hbuf[pl.ds(2 * j + 1, N, stride=8), :])
            right = jnp.concatenate(
                [jnp.concatenate([h0, h1], axis=1), jnp.concatenate([l0, l1], axis=1)], axis=0
            )
            both = dot(fz[...], right)
            both = both[:N] + both[N:]
            keep = keep_of(j)
            keep = keep + pltpu.roll(keep, KEPT, axis=1)
            for b in range(BANDS):
                cos_part = both[:KEPT, b * N : (b + 1) * N]
                sin_part = both[KEPT:, b * N : (b + 1) * N]
                applied = cos_part - turn_sign * pltpu.roll(sin_part, KEPT, axis=1)
                out[b, j] = keep * (factor * applied) + base[b, j]

    with jax.named_scope("wait_sends"):

        @pl.when(active)
        def _():

            @pl.when(my_z < 2)
            def _():
                v_last(5, 24).wait_send()
                v_last(6, 48).wait_send()

            @pl.when(my_z >= 2)
            def _():
                v_last(5, 8).wait_send()
                v_last(6, 96).wait_send()
                v_last(8, 64).wait_send()

            for c in range(PLANES):
                awaited(sbuf.at[pl.ds(0, 8 * peers_with(c)), :], fsend.at[c], frecv.at[c]).wait_send()
                awaited(gbuf.at[c, pl.ds(0, 8 * (ACTIVE - 1)), :], gsend.at[c], grecv.at[c]).wait_send()

        @pl.when(jnp.logical_not(active))
        def _():
            v_handed.wait_send()
            for c in range(FEW):
                awaited(gbuf.at[c], gsend.at[c], grecv.at[c]).wait_send()

        def v_sent(planes):
            @pl.when(early)
            def _():
                v_wait(planes, 4, 48).wait_send()

            @pl.when(jnp.logical_not(early))
            def _():
                v_wait(planes, 4, 96).wait_send()

            @pl.when(tardy)
            def _():
                awaited(v_part(planes, pl.ds(0, 8)), vsend.at[my_z_turn], vrecv.at[4]).wait_send()
                v_wait(planes, 7, 64).wait_send()

            @pl.when(jnp.logical_not(tardy))
            def _():
                awaited(v_part(planes, pl.ds(0, 24)), vsend.at[my_z_turn], vrecv.at[4]).wait_send()

        for_kind(v_sent)


def expand(packed, out, obuf, sem):
    me = lax.axis_index("fft")
    active = jnp.logical_or(me < ACTIVE // 2, me >= FFT - ACTIVE // 2)
    lane = lax.broadcasted_iota(jnp.int32, (KEPT, N), 1)
    natural = jnp.logical_or(lane < HALF, lane >= N - HALF)
    copies = [pltpu.make_async_copy(obuf.at[:, b], out.at[:, b], sem.at[b]) for b in range(BANDS)]

    @pl.when(active)
    def _():
        for b in range(BANDS):
            for j in range(4):
                both = packed[b, j]
                for t, part in enumerate((both, pltpu.roll(both, KEPT, axis=1))):
                    part = jnp.where(natural, part, 0.0)
                    obuf[t, b, j, :HALF, :] = part[:HALF]
                    obuf[t, b, j, HALF : N - HALF, :] = jnp.zeros((KEPT, N), jnp.float32)
                    obuf[t, b, j, N - HALF :, :] = part[HALF:]
            copies[b].start()

    @pl.when(jnp.logical_not(active))
    def _():
        obuf[...] = jnp.zeros_like(obuf)
        for copy in copies:
            copy.start()

    for copy in copies:
        copy.wait()


def local(tables, wave, previous, potential, column_extent, metric, center, halfwidth):
    any_spec = pl.BlockSpec(memory_space=pltpu.HBM)
    vmem_spec = pl.BlockSpec(memory_space=pltpu.VMEM)
    smem_spec = pl.BlockSpec(memory_space=pltpu.SMEM)
    f32, bf16 = jnp.float32, jnp.bfloat16
    dma = pltpu.SemaphoreType.DMA
    packed = pl.pallas_call(
        kernel,
        out_shape=pltpu.VMEM((BANDS, 4, KEPT, N), f32),
        in_specs=[any_spec] * 5 + [smem_spec] * 2 + [any_spec] * 6,
        out_specs=vmem_spec,
        scratch_shapes=[
            pltpu.VMEM((4, N), jnp.int32),
            pltpu.SMEM((3,), f32),
            pltpu.VMEM((2, BANDS, 4, KEPT, N), f32),
            pltpu.VMEM((2, BANDS, 4, KEPT, N), f32),
            pltpu.VMEM((PLANES, N, N), f32),
            *[pltpu.VMEM(table.shape, bf16) for table in tables],
            pltpu.VMEM((32, N), f32),
            pltpu.VMEM((4, 2 * N, 2 * N), bf16),
            pltpu.VMEM((8 * N, N), f32),
            pltpu.VMEM((PLANES, N, N), f32),
            pltpu.VMEM((N, N), f32),
            pltpu.VMEM((N, N), f32),
            pltpu.VMEM((PLANES, BANDS, N, 2 * N), f32),
            pltpu.VMEM((N, 2 * N), bf16),
            pltpu.VMEM((N, 2 * N), bf16),
            pltpu.VMEM((PLANES, N, N), f32),
            pltpu.VMEM((8 * N, N), f32),
            pltpu.VMEM((BANDS, 4, KEPT, N), f32),
            dma((BANDS, 2)),
            dma((2,)),
            dma((6,)),
            dma((3,)),
            dma((PLANES,)),
            dma((PLANES,)),
            dma((PLANES,)),
            dma((PLANES,)),
            dma((9,)),
            dma((9,)),
            dma,
            dma,
            pltpu.SemaphoreType.REGULAR((5,)),
        ],
        compiler_params=pltpu.CompilerParams(
            collective_id=0, has_side_effects=True, vmem_limit_bytes=24 * 1024 * 1024
        ),
    )(
        *[
            pltpu.with_memory_space_constraint(value, pltpu.HBM)
            for value in (wave, previous, potential.reshape(32, N), column_extent, metric)
        ],
        center,
        halfwidth,
        *[pltpu.with_memory_space_constraint(table, pltpu.HBM) for table in tables],
    )
    return pl.pallas_call(
        expand,
        out_shape=jax.ShapeDtypeStruct(wave.shape, f32),
        in_specs=[vmem_spec],
        out_specs=any_spec,
        scratch_shapes=[pltpu.VMEM((2, BANDS, 4, N, N), f32), dma((BANDS,))],
        compiler_params=pltpu.CompilerParams(vmem_limit_bytes=8 * 1024 * 1024),
    )(packed)


def solution(mesh):
    tables = [jnp.asarray(table) for table in make_tables()]
    in_specs = (
        P(None, "band", "fft", None, None),
        P(None, "band", "fft", None, None),
        P("band", "fft", None),
        P("fft", None),
        P(),
        P(),
        P(),
    )
    out_specs = P(None, "band", "fft", None, None)
    return jax.shard_map(
        functools.partial(local, tables), mesh=mesh, in_specs=in_specs, out_specs=out_specs, check_vma=False
    )
```

```python
import functools
import math

import jax
import jax.numpy as jnp
import numpy as np
from jax import lax
from jax.experimental import pallas as pl
from jax.experimental.pallas import tpu as pltpu
from jax.sharding import PartitionSpec as P

N = 128
KEPT = 64
HALF = KEPT // 2
FFT = 32
ACTIVE = 16
BANDS = 2
PLANES = 5
FEW = 3
FIRST = (0,)
MESH = pl.DeviceIdType.MESH


def kept_indices():
    return np.concatenate([np.arange(HALF), np.arange(N - HALF, N)])


def cos_sin(rows, cols):
    angles = (np.outer(rows, cols) % N) * (2.0 * math.pi / N)
    return np.cos(angles), np.sin(angles)


def split(table):
    high = table.astype(jnp.bfloat16)
    low = (table - high.astype(np.float64)).astype(jnp.bfloat16)
    return high, low


def stacked(cosine, sine):
    cos_high, cos_low = split(cosine)
    sin_high, sin_low = split(sine)
    zero = np.zeros_like(cos_low)
    return np.concatenate(
        [
            np.concatenate([cos_high, cos_high], axis=1),
            np.concatenate([sin_high, sin_high], axis=1),
            np.concatenate([cos_low, zero], axis=1),
            np.concatenate([sin_low, zero], axis=1),
        ],
        axis=0,
    )


def make_tables():
    grid = np.arange(N)
    kept = kept_indices()
    slots = np.arange(ACTIVE)
    first_gx = 4 * np.where(slots < ACTIVE // 2, slots, slots + FFT - ACTIVE)

    cosine, sine = cos_sin(grid, kept)
    high, low = split(np.concatenate([cosine, sine], axis=1))
    zero = np.zeros_like(low)
    inverse_z = np.concatenate([np.concatenate([high, high], axis=1), np.concatenate([low, zero], axis=1)], axis=0)

    lanes = np.arange(N)
    natural = (lanes < HALF) | (lanes >= N - HALF)
    gy = np.where(natural, lanes, (lanes + KEPT) % N)
    cosine, sine = cos_sin(gy, grid)
    pick = natural[:, None]
    table = np.concatenate([np.where(pick, cosine, -sine), np.where(pick, sine, cosine)], axis=1)
    high, low = split(table)
    inverse_y = np.concatenate([high, high, low], axis=0)

    order = (first_gx[:, None] + np.arange(4)[None, :]).reshape(-1)
    cosine, sine = cos_sin(grid, order)
    cos_high, cos_low = split(cosine)
    sin_high, sin_low = split(sine)
    zero = np.zeros_like(cos_low)
    inverse_x = np.concatenate(
        [
            np.concatenate([cos_high, sin_high, cos_high, sin_high], axis=1),
            np.concatenate([cos_low, sin_low, zero, zero], axis=1),
        ],
        axis=0,
    )

    cosine, sine = cos_sin(order, grid)
    forward_x = stacked(cosine / N, sine / N)

    cosine, sine = cos_sin(grid, gy)
    pick = natural[None, :]
    table = np.concatenate([np.where(pick, cosine, -sine), np.where(pick, sine, cosine)], axis=0) / N
    forward_y = np.concatenate(split(table), axis=1)

    cosine, sine = cos_sin(kept, grid)
    forward_z = stacked(cosine / N, sine / N)
    return [inverse_z, inverse_y, inverse_x, forward_x, forward_y, forward_z]


def halves(value):
    high = value.astype(jnp.bfloat16)
    low = (value - high.astype(jnp.float32)).astype(jnp.bfloat16)
    return high, low


def dot(left, right):
    return jnp.dot(left, right, preferred_element_type=jnp.float32)


def kernel(
    wave,
    previous,
    potential,
    extent_hbm,
    metric_hbm,
    center,
    halfwidth,
    iz_hbm,
    iy_hbm,
    ix_hbm,
    fx_hbm,
    fy_hbm,
    fz_hbm,
    out,
    extent,
    metric,
    wbuf,
    pbuf,
    vbuf,
    iz,
    iy,
    ix,
    fx,
    fy,
    fz,
    vown,
    zboth,
    sbuf,
    rbuf,
    yre,
    yim,
    fbuf,
    qhigh,
    qlow,
    gbuf,
    hbuf,
    base,
    wsem,
    psem,
    tsem,
    lsem,
    fsend,
    frecv,
    gsend,
    grecv,
    vsend,
    vrecv,
    esend,
    erecv,
    ready,
):
    me = lax.axis_index("fft")
    band = lax.axis_index("band")
    my_x, my_z = lax.div(band, 4), lax.rem(band, 4)
    my_y, my_low = lax.div(me, 4), lax.rem(me, 4)
    active = jnp.logical_or(me < ACTIVE // 2, me >= FFT - ACTIVE // 2)
    slot = jnp.where(me < ACTIVE // 2, me, me - (FFT - ACTIVE))
    lows = [my_low] + [lax.rem(my_low + i, 4) for i in (1, 2, 3)]
    rows_of_peers = [(lax.rem(my_y + dy, 8), lows) for dy in (4, 3, 5, 2, 6, 1, 7)] + [(my_y, lows[1:])]
    z_peers = [lax.rem(my_z + d, 4) for d in (2, 1, 3)]
    x_peers = [lax.rem(my_x + d, 4) for d in (2, 1, 3)]

    def hello(semaphore, where):
        pl.semaphore_signal(semaphore, inc=1, device_id=where, device_id_type=MESH)

    def wait_for(semaphore, count):
        @pl.when(count > 0)
        def _():
            pl.semaphore_wait(semaphore, count)

    def turn_of(y, place):
        usual = 4 * jnp.where(y < 4, y, 11 - y) + place
        return jnp.where(jnp.logical_and(band == 0, usual == 0), FFT, usual)

    my_turn = turn_of(my_y, my_low)
    earlier = jnp.where(band == 0, my_turn - 1, my_turn)
    z_shift = jnp.where(jnp.logical_and(me == 0, my_x == 0), 1, 0)
    x_shift = jnp.where(jnp.logical_and(me == 0, my_z == 0), 1, 0)

    def z_turn(z):
        return jnp.where(z < z_shift, 1, jnp.where(z == 1, 1 - z_shift, z))

    def x_turn(x):
        return jnp.where(x < x_shift, 3, x - x_shift)

    my_z_turn, my_x_turn = z_turn(my_z), x_turn(my_x)

    late = jnp.logical_and(band == 0, me == 0)
    side_2 = jnp.logical_and(my_y >= 2, my_y < 4)
    side_6 = my_y >= 6
    later_rows = jnp.where(late, 0, jnp.where(my_y == 0, 12, jnp.where(my_y == 1, 8, jnp.where(my_y == 7, 4, 0))))

    my_row = jnp.where(my_y < 4, my_y, 11 - my_y)
    y_order = (4, 5, 6, 3, 7, 2, 1, 0)

    def greet(semaphore, later):
        def to(y, line, core, semaphore):
            place = 2 * line + core
            if y == 0 and core == 0 and not later:

                @pl.when(jnp.logical_or(band != 0, line != 0))
                def _():
                    hello(semaphore, {"fft": y * 4 + place})
            else:
                hello(semaphore, {"fft": y * 4 + place})

        for y in y_order:
            y_row = y if y < 4 else 11 - y
            near = y_row > my_row if later else y_row < my_row
            if later and y >= 6:
                near = near & jnp.logical_not(side_2)
            if not later and 2 <= y < 4:
                near = near & jnp.logical_not(side_6)

            def row(semaphore):
                for line in range(2):
                    for core in range(2):
                        to(y, line, core, semaphore)

            if later or 2 <= y < 6:
                pl.when(near)(lambda: row(semaphore))
            else:
                pl.when(near & active)(lambda: row(ready.at[5]))
                pl.when(near & jnp.logical_not(active))(lambda: row(semaphore))

        for place in range(4):

            @pl.when(place > my_low if later else place < my_low)
            def _():
                if place > 0:
                    hello(semaphore, {"fft": my_y * 4 + place})
                else:

                    @pl.when(jnp.logical_or(band != 0, my_y > 0))
                    def _():
                        hello(semaphore, {"fft": my_y * 4})

    def greet_all(semaphore):
        for y in range(FFT // 4):
            for place in range(4):
                if y + place > 0:
                    hello(semaphore, {"fft": y * 4 + place})

    def is_late_row(y):
        return jnp.logical_and(band == 0, y == 0)

    load_v = pltpu.make_async_copy(potential, vown, lsem.at[0])
    load_v.start()
    barrier = pltpu.get_barrier_semaphore()
    direct = jnp.logical_not(active)
    early = jnp.logical_and(direct, my_z < 2)
    tardy = jnp.logical_and(direct, my_z >= 2)

    @pl.when(jnp.logical_not(late))
    def _():
        greet(barrier, True)

    @pl.when(jnp.logical_and(band == 0, me > 0))
    def _():
        hello(barrier, {"fft": 0})

    @pl.when(my_z < 2)
    def _():
        for z in (2, 3):
            for x in x_peers:
                hello(barrier, {"band": x * 4 + z})

    for z in z_peers:

        @pl.when(z_turn(z) > my_z_turn)
        def _():
            hello(barrier, {"band": my_x * 4 + z})

    for x in x_peers:

        @pl.when(x_turn(x) > my_x_turn)
        def _():
            hello(barrier, {"band": x * 4 + my_z})

    def wave_copies(b):
        return [
            pltpu.make_async_copy(
                wave.at[:, b, :, pl.ds(h * (N - HALF), HALF), :],
                wbuf.at[:, b, :, pl.ds(h * HALF, HALF), :],
                wsem.at[b, h],
            )
            for h in range(2)
        ]

    previous_copies = [
        pltpu.make_async_copy(
            previous.at[:, :, :, pl.ds(h * (N - HALF), HALF), :],
            pbuf.at[:, :, :, pl.ds(h * HALF, HALF), :],
            psem.at[h],
        )
        for h in range(2)
    ]
    small_refs = ((extent_hbm, extent), (metric_hbm, metric))
    small_copies = [pltpu.make_async_copy(a, b, lsem.at[i + 1]) for i, (a, b) in enumerate(small_refs)]
    table_refs = ((iz_hbm, iz), (iy_hbm, iy), (ix_hbm, ix), (fx_hbm, fx), (fy_hbm, fy), (fz_hbm, fz))
    table_copies = [pltpu.make_async_copy(a, b, tsem.at[i]) for i, (a, b) in enumerate(table_refs)]

    for copy in small_copies:
        copy.start()

    @pl.when(active)
    def _():
        for b in range(BANDS):
            for copy in wave_copies(b):
                copy.start()

    for copy in table_copies:
        copy.start()

    @pl.when(active)
    def _():
        for copy in previous_copies:
            copy.start()

    row = lax.broadcasted_iota(jnp.int32, (KEPT, N), 0)
    lane = lax.broadcasted_iota(jnp.int32, (KEPT, N), 1)
    natural = jnp.logical_or(lane < HALF, lane >= N - HALF)
    signed_gz = jnp.where(row < HALF, row, row - KEPT)
    place_gy = jnp.where(natural, lane, jnp.where(lane < KEPT, lane + KEPT, lane - KEPT))
    signed_gy = jnp.where(place_gy < N // 2, place_gy, place_gy - N)
    turn_sign = jnp.where(natural, -1.0, 1.0).astype(jnp.float32)

    def is_active(y):
        return jnp.logical_or(y < 2, y >= 6)

    def partner(y):
        return lax.rem(jnp.where(jnp.logical_or(y < 2, jnp.logical_or(y == 4, y == 5)), y + 2, y + 6), 8)

    def plane_of(y, place, c):
        if c < 4:
            return 4 * (y * 4 + place) + c
        if isinstance(y, int):
            return 4 * ((y + 2 if y < 2 else y - 2) * 4 + place) + 3
        return 4 * (partner(y) * 4 + place) + 3

    def keep_of(j):
        return (jnp.abs(signed_gz) <= extent[pl.ds(j, 1), :]).astype(jnp.float32)

    def both_parts(keep, real, imag):
        return keep * real + pltpu.roll(keep * imag, KEPT, axis=1)

    def to_planes():
        for b in range(BANDS):
            for copy in wave_copies(b):
                copy.wait()
        for j in range(4):
            keep = keep_of(j)
            for b in range(BANDS):
                packed = both_parts(keep, wbuf[0, b, j], wbuf[1, b, j])
                turned = pltpu.roll(packed, KEPT, axis=1) * turn_sign
                for t, part in enumerate((packed, turned)):
                    high, low = halves(part)
                    zboth[j, t * KEPT : (t + 1) * KEPT, b * N : (b + 1) * N] = high
                    zboth[j, N + t * KEPT : N + (t + 1) * KEPT, b * N : (b + 1) * N] = low
            both = dot(iz[...], zboth[j])
            both = both[:N] + both[N:]
            for b in range(BANDS):
                sbuf[pl.ds(2 * j + b, N, stride=8), :] = both[:, b * N : (b + 1) * N]
        for c in range(PLANES):
            mine = sbuf[pl.ds(pl.multiple_of(plane_of(my_y, my_low, c) * 8, 8), 8), :]
            rbuf[c, pl.ds(pl.multiple_of(slot * 8, 8), 8), :] = mine

    def scale():
        return jnp.full((1, N), 2.0, jnp.float32) / jnp.full((1, N), halfwidth[0], jnp.float32)

    def the_rest():
        for copy in previous_copies:
            copy.wait()
        step_z = (2.0 * math.pi / N) * signed_gz.astype(jnp.float32)
        step_y = (2.0 * math.pi / N) * signed_gy.astype(jnp.float32)
        plane_kinetic = metric[2] * (step_z * step_z) + metric[1] * (step_y * step_y)
        factor = scale()
        for j in range(4):
            gx = me * 4 + j
            signed_gx = jnp.where(gx < N // 2, gx, gx - N).astype(jnp.float32)
            step_x = (2.0 * math.pi / N) * signed_gx
            weight = factor * (0.5 * (metric[0] * (step_x * step_x) + plane_kinetic) - center[0])
            keep = keep_of(j)
            for b in range(BANDS):
                coefficient = both_parts(keep, wbuf[0, b, j], wbuf[1, b, j])
                base[b, j] = weight * coefficient - both_parts(keep, pbuf[0, b, j], pbuf[1, b, j])

    def send_plane(c, y, place):
        pltpu.make_async_remote_copy(
            src_ref=sbuf.at[pl.ds(pl.multiple_of(plane_of(y, place, c) * 8, 8), 8), :],
            dst_ref=rbuf.at[c, pl.ds(pl.multiple_of(slot * 8, 8), 8), :],
            send_sem=fsend.at[c],
            recv_sem=frecv.at[c],
            device_id={"fft": y * 4 + place},
            device_id_type=MESH,
        ).start()

    def to_others(y, send):
        @pl.when(my_y == y)
        def _():
            for place in lows[1:]:
                send(y, place)

        @pl.when(my_y != y)
        def _():
            for place in lows:
                send(y, place)

    def send_row(c, y):
        def unless_late(place):
            @pl.when(jnp.logical_and(place > 0, y * 4 + place != me))
            def _():
                send_plane(c, y, place)

        def send(y, place):
            send_plane(c, y, place)

        if y > 0:
            to_others(y, send)
        else:

            @pl.when(band == 0)
            def _():
                for place in lows:
                    unless_late(place)

            @pl.when(band != 0)
            def _():
                to_others(y, send)

    def send_rows(planes, rows):
        for c in planes:
            for y in rows:
                if 2 <= y < 6:
                    for place in lows:
                        send_plane(c, y, place)
                else:
                    send_row(c, y)

    def send_columns(c):
        plane = plane_of(my_y, my_low, c)

        def send(y, place):
            first = (y if y < 2 else y - 4) * 4
            pltpu.make_async_remote_copy(
                src_ref=gbuf.at[c, pl.ds(pl.multiple_of((first + place) * 8, 8), 8), :],
                dst_ref=hbuf.at[pl.ds(pl.multiple_of(plane * 8, 8), 8), :],
                send_sem=gsend.at[c],
                recv_sem=grecv.at[c],
                device_id={"fft": y * 4 + place},
                device_id_type=MESH,
            ).start()

        @pl.when(active)
        def _():
            for y in (7, 0, 6, 1):
                to_others(y, send)

        if c < FEW:

            @pl.when(jnp.logical_not(active))
            def _():
                for y in (7, 0, 6, 1):
                    for place in lows:
                        send(y, place)

    def awaited(ref, send, recv):
        return pltpu.make_async_remote_copy(
            src_ref=ref, dst_ref=ref, send_sem=send, recv_sem=recv, device_id={"fft": me}, device_id_type=MESH
        )

    def send_v(where, phase, peer):
        pltpu.make_async_remote_copy(
            src_ref=where,
            dst_ref=where,
            send_sem=vsend.at[phase],
            recv_sem=vrecv.at[phase],
            device_id={"band": peer},
            device_id_type=MESH,
        ).start()

    my_rows = pl.ds(pl.multiple_of(band * 8, 8), 8)

    def v_part(planes, rows):
        return vbuf.at[pl.ds(0, planes), rows, :]

    def v_rows(z):
        return pl.ds(pl.multiple_of(my_x * 32 + z * 8, 8), 8)

    def for_kind(function):
        pl.when(active)(lambda: function(4))
        pl.when(jnp.logical_not(active))(lambda: function(FEW))

    def takes_z(z):
        return jnp.logical_not(jnp.logical_and(tardy, z < 2))

    def send_v_along_z(z, turn):
        @pl.when(takes_z(z))
        def _():
            for_kind(lambda planes: send_v(v_part(planes, my_rows), turn, my_x * 4 + z))

    def v_along_z(planes, turn):
        return awaited(v_part(planes, pl.ds(0, 8)), vsend.at[turn], vrecv.at[turn])

    def send_v_along_x(z):
        for x in x_peers:
            for_kind(lambda planes: send_v(v_part(planes, v_rows(z)), 4, x * 4 + my_z))

    def send_v_directly(part, phase):
        for z in range(2):
            for x in x_peers + [my_x]:
                send_v(part, phase, x * 4 + z)

    def v_wait(planes, phase, rows):
        return awaited(v_part(planes, pl.ds(0, rows)), vsend.at[phase], vrecv.at[phase])

    def v_last(phase, rows):
        return awaited(vbuf.at[4, pl.ds(0, rows), :], vsend.at[phase], vrecv.at[phase])

    v_handed = pltpu.make_async_remote_copy(
        src_ref=vbuf.at[3, my_rows, :],
        dst_ref=vbuf.at[4, my_rows, :],
        send_sem=esend,
        recv_sem=erecv,
        device_id={"fft": partner(my_y) * 4 + my_low},
        device_id_type=MESH,
    )

    def field(c):
        with jax.named_scope(f"wait_planes{c}"):

            @pl.when(active)
            def _():
                awaited(rbuf.at[c, pl.ds(0, 8 * (ACTIVE - 1)), :], fsend.at[c], frecv.at[c]).wait_recv()

            if c < FEW:

                @pl.when(jnp.logical_not(active))
                def _():
                    awaited(rbuf.at[c], fsend.at[c], frecv.at[c]).wait_recv()

        high, low = halves(rbuf[c])
        plane = dot(jnp.concatenate([high, low, high], axis=1), iy[...])
        yre[...] = plane[:, :N]
        yim[...] = plane[:, N:]
        for b in range(BANDS):
            rh, rl = halves(yre[pl.ds(b, KEPT, stride=2), :])
            ih, il = halves(yim[pl.ds(b, KEPT, stride=2), :])
            right = jnp.concatenate(
                [
                    jnp.concatenate([rh, ih], axis=1),
                    jnp.concatenate([-ih, rh], axis=1),
                    jnp.concatenate([rl, il], axis=1),
                    jnp.concatenate([-il, rl], axis=1),
                ],
                axis=0,
            )
            both = dot(ix[...], right)
            fbuf[c, b] = both[:N] + both[N:]

    def back(c):
        if c == 0:
            with jax.named_scope("wait_v"):

                def arrived(planes):
                    @pl.when(early)
                    def _():
                        v_wait(planes, 4, 48).wait_recv()
                        v_wait(planes, 7, 64).wait_recv()

                    @pl.when(jnp.logical_not(early))
                    def _():
                        v_wait(planes, 4, 96).wait_recv()

                for_kind(arrived)
        if c == 4:
            with jax.named_scope("wait_v4"):


                @pl.when(my_z < 2)
                def _():
                    v_last(6, 48).wait_recv()
                    v_last(8, 64).wait_recv()

                @pl.when(my_z >= 2)
                def _():
                    v_last(6, 96).wait_recv()

        local_v = vbuf[c]
        for b in range(BANDS):
            rh, rl = halves(fbuf[c, b, :, :N] * local_v)
            ih, il = halves(fbuf[c, b, :, N:] * local_v)
            right = jnp.concatenate(
                [jnp.concatenate([rh, ih], axis=1), jnp.concatenate([rl, il], axis=1)], axis=0
            )
            both = dot(fx[...], right)
            both = both[:N] + both[N:]
            cos_part, sin_part = both[:KEPT], both[KEPT:]
            rows = slice(b * KEPT, (b + 1) * KEPT)
            high, low = halves(cos_part[:, :N] + sin_part[:, N:])
            qhigh[rows, :N] = high
            qlow[rows, :N] = low
            high, low = halves(cos_part[:, N:] - sin_part[:, :N])
            qhigh[rows, N:] = high
            qlow[rows, N:] = low
        wide = dot(qhigh[...], fy[...])
        packed = wide[:, :N] + wide[:, N:] + dot(qlow[...], fy[:, :N])
        for b in range(BANDS):
            gbuf[c, pl.ds(b, KEPT, stride=2), :] = packed[b * KEPT : (b + 1) * KEPT]
        with jax.named_scope(f"send_columns{c}"):
            send_columns(c)

        def keep_mine():
            mine = gbuf[c, pl.ds(pl.multiple_of(slot * 8, 8), 8), :]
            hbuf[pl.ds(pl.multiple_of(plane_of(my_y, my_low, c) * 8, 8), 8), :] = mine

        if c < FEW:
            pl.when(active)(keep_mine)
        else:
            keep_mine()

    with jax.named_scope("barrier"):
        wait_for(barrier, earlier + my_z_turn + my_x_turn + jnp.where(my_z >= 2, 6, 0) - jnp.where(side_6, 8, 0))
        load_v.wait()
        for c in range(4):
            vbuf[c, my_rows, :] = vown[pl.ds(c, 8, stride=4), :]

    @pl.when(tardy)
    def _():
        send_v_directly(v_part(FEW, my_rows), 7)

    @pl.when(late)
    def _():
        greet_all(ready.at[3])

    @pl.when(jnp.logical_not(late))
    def _():
        greet(ready.at[2], False)

    waits_for_first = jnp.logical_and(band == 0, me == 8)

    @pl.when(jnp.logical_not(jnp.logical_or(active, waits_for_first)))
    def _():
        v_handed.start()


    for z in z_peers:

        @pl.when(z_turn(z) < my_z_turn)
        def _():
            hello(ready.at[6 + my_z_turn], {"band": my_x * 4 + z})
            send_v_along_z(z, my_z_turn)

    for x in x_peers:

        @pl.when(x_turn(x) < my_x_turn)
        def _():
            hello(ready.at[1], {"band": x * 4 + my_z})

    for copy in small_copies:
        copy.wait()
    table_copies[0].wait()

    @pl.when(active)
    def _():
        with jax.named_scope("planes"):
            to_planes()

        with jax.named_scope("send_first"):

            @pl.when(my_y == 1)
            def _():
                send_rows(FIRST, (0,))

            @pl.when(my_y == 7)
            def _():
                send_rows(FIRST, (1, 0))

            @pl.when(my_y == 6)
            def _():
                send_rows(FIRST, (1, 0, 7))

    def hand_on(z, later):
        @pl.when(active & (z_turn(z) > my_z_turn if later else z_turn(z) < my_z_turn) & jnp.logical_not((my_z >= 2) & (z < 2)))
        def _():
            send_v(vbuf.at[4, my_rows, :], 5, my_x * 4 + z)

    @pl.when(jnp.logical_and(active, jnp.logical_not(late)))
    def _():
        with jax.named_scope("wait_handed"):
            v_handed.wait_recv()
        for z in z_peers:
            hand_on(z, False)

        @pl.when(my_z >= 2)
        def _():
            send_v_directly(vbuf.at[4, my_rows, :], 8)

    def own_along_x():
        with jax.named_scope("wait_x"):
            wait_for(ready.at[1], 3 - my_x_turn)
        send_v_along_x(my_z)

    def z_of(turn):
        return jnp.abs(turn - z_shift) if turn < 2 else turn

    def reach_z(turn):
        @pl.when(turn > my_z_turn)
        def _():
            with jax.named_scope(f"wait_z{turn}"):
                pl.semaphore_wait(ready.at[6 + turn], 1)
            send_v_along_z(z_of(turn), my_z_turn)

            @pl.when(jnp.logical_not(late))
            def _():
                hand_on(z_of(turn), True)

    def forward_v(turn):
        @pl.when(turn != my_z_turn if turn < 2 else jnp.logical_and(turn != my_z_turn, jnp.logical_not(early)))
        def _():
            with jax.named_scope(f"wait_vz{turn}"):
                for_kind(lambda planes: v_along_z(planes, turn).wait_recv())
            send_v_along_x(z_of(turn))

    def know_late():
        @pl.when(jnp.logical_and(band == 0, me > 0))
        def _():
            with jax.named_scope("wait_late"):
                pl.semaphore_wait(ready.at[3], 1)

            @pl.when(me == 8)
            def _():
                v_handed.start()

            @pl.when(active)
            def _():
                for c in range(PLANES):
                    send_plane(c, 0, 0)

    @pl.when(active)
    def _():
        own_along_x()

    @pl.when(jnp.logical_not(active))
    def _():
        own_along_x()
        reach_z(1)
        forward_v(0)
        forward_v(1)
        know_late()
        reach_z(2)
        reach_z(3)
        forward_v(2)
        forward_v(3)

    with jax.named_scope("wait_rows"):
        wait_for(ready.at[5], later_rows)

    with jax.named_scope("send_rows"):

        @pl.when(my_y == 0)
        def _():
            send_rows(FIRST, (6, 7, 1))

        @pl.when(my_y == 1)
        def _():
            send_rows(FIRST, (6, 7))

        @pl.when(my_y == 7)
        def _():
            send_rows(FIRST, (6,))

    with jax.named_scope("wait_group"):
        wait_for(
            ready.at[2],
            jnp.where(late, 0, jnp.where(band == 0, FFT - 2, FFT - 1) - earlier - jnp.where(side_2, 8, 0) - later_rows),
        )

    @pl.when(my_y == 1)
    def _():
        for y in (7, 6):
            hello(ready.at[4], {"fft": y * 4 + my_low})

    with jax.named_scope("send"):

        rest = [c for c in range(PLANES) if c not in FIRST]

        def own_row(planes):
            for y in (0, 1, 6, 7):

                @pl.when(my_y == y)
                def _():
                    send_rows(planes, (y,))

        @pl.when(my_y < 2)
        def _():
            send_rows((0,), (4, 3, 5, 2))
            own_row(FIRST)
            send_rows((1,), (4, 3, 5, 2))
            send_rows(rest[:1], (6, 7, 1, 0))
            send_rows((2,), (4, 3, 5, 2))
            send_rows(rest[1:], (6, 7, 1, 0))

        @pl.when(side_6)
        def _():
            send_rows((0,), (4, 5))
            own_row(FIRST)
            pl.semaphore_wait(ready.at[4], 1)
            send_rows((0,), (3, 2))
            send_rows((1,), (3, 4, 2, 5))
            send_rows(rest[:1], (1, 0, 7, 6))
            send_rows((2,), (3, 4, 2, 5))
            send_rows(rest[1:], (1, 0, 7, 6))

    @pl.when(active)
    def _():
        reach_z(1)
        forward_v(0)
        forward_v(1)
        know_late()
        reach_z(2)
        reach_z(3)
        with jax.named_scope("the_rest"):
            the_rest()
        forward_v(2)
        forward_v(3)

        @pl.when(late)
        def _():
            v_handed.wait_recv()
            for z in z_peers:
                hand_on(z, False)
                hand_on(z, True)

    for copy in table_copies[1:]:
        copy.wait()

    def forward_last():
        with jax.named_scope("wait_vlast"):

            def forward(blocks):
                v_last(5, 8 * blocks - 8 if blocks > 2 else 8).wait_recv()
                for x in x_peers:
                    send_v(vbuf.at[4, pl.ds(pl.multiple_of(my_x * 32, 32), 8 * blocks), :], 6, x * 4 + my_z)

            pl.when(my_z < 2)(lambda: forward(2))
            pl.when(my_z >= 2)(lambda: forward(4))

    for c in range(FEW):
        field(c)
        back(c)
        if c == 0:
            pl.when(active)(forward_last)

    def peers_with(c):
        return FFT - 1 if c < FEW else ACTIVE - 1

    @pl.when(active)
    def _():
        for c in range(FEW, PLANES):
            field(c)
            back(c)
        factor = scale()
        for c in range(PLANES):
            with jax.named_scope(f"wait_columns{c}"):
                awaited(hbuf.at[pl.ds(0, 8 * peers_with(c)), :], gsend.at[c], grecv.at[c]).wait_recv()
        for j in range(4):
            h0, l0 = halves(hbuf[pl.ds(2 * j, N, stride=8), :])
            h1, l1 = halves(hbuf[pl.ds(2 * j + 1, N, stride=8), :])
            right = jnp.concatenate(
                [jnp.concatenate([h0, h1], axis=1), jnp.concatenate([l0, l1], axis=1)], axis=0
            )
            both = dot(fz[...], right)
            both = both[:N] + both[N:]
            keep = keep_of(j)
            keep = keep + pltpu.roll(keep, KEPT, axis=1)
            for b in range(BANDS):
                cos_part = both[:KEPT, b * N : (b + 1) * N]
                sin_part = both[KEPT:, b * N : (b + 1) * N]
                applied = cos_part - turn_sign * pltpu.roll(sin_part, KEPT, axis=1)
                out[b, j] = keep * (factor * applied) + base[b, j]

    with jax.named_scope("wait_sends"):

        @pl.when(active)
        def _():

            @pl.when(my_z < 2)
            def _():
                v_last(5, 24).wait_send()
                v_last(6, 48).wait_send()

            @pl.when(my_z >= 2)
            def _():
                v_last(5, 8).wait_send()
                v_last(6, 96).wait_send()
                v_last(8, 64).wait_send()

            for c in range(PLANES):
                awaited(sbuf.at[pl.ds(0, 8 * peers_with(c)), :], fsend.at[c], frecv.at[c]).wait_send()
                awaited(gbuf.at[c, pl.ds(0, 8 * (ACTIVE - 1)), :], gsend.at[c], grecv.at[c]).wait_send()

        @pl.when(jnp.logical_not(active))
        def _():
            v_handed.wait_send()
            for c in range(FEW):
                awaited(gbuf.at[c], gsend.at[c], grecv.at[c]).wait_send()

        def v_sent(planes):
            @pl.when(early)
            def _():
                v_wait(planes, 4, 48).wait_send()

            @pl.when(jnp.logical_not(early))
            def _():
                v_wait(planes, 4, 96).wait_send()

            @pl.when(tardy)
            def _():
                awaited(v_part(planes, pl.ds(0, 8)), vsend.at[my_z_turn], vrecv.at[4]).wait_send()
                v_wait(planes, 7, 64).wait_send()

            @pl.when(jnp.logical_not(tardy))
            def _():
                awaited(v_part(planes, pl.ds(0, 24)), vsend.at[my_z_turn], vrecv.at[4]).wait_send()

        for_kind(v_sent)


def expand(packed, out, obuf, sem):
    me = lax.axis_index("fft")
    active = jnp.logical_or(me < ACTIVE // 2, me >= FFT - ACTIVE // 2)
    lane = lax.broadcasted_iota(jnp.int32, (KEPT, N), 1)
    natural = jnp.logical_or(lane < HALF, lane >= N - HALF)
    copies = [pltpu.make_async_copy(obuf.at[:, b], out.at[:, b], sem.at[b]) for b in range(BANDS)]

    @pl.when(active)
    def _():
        for b in range(BANDS):
            for j in range(4):
                both = packed[b, j]
                for t, part in enumerate((both, pltpu.roll(both, KEPT, axis=1))):
                    part = jnp.where(natural, part, 0.0)
                    obuf[t, b, j, :HALF, :] = part[:HALF]
                    obuf[t, b, j, HALF : N - HALF, :] = jnp.zeros((KEPT, N), jnp.float32)
                    obuf[t, b, j, N - HALF :, :] = part[HALF:]
            copies[b].start()

    @pl.when(jnp.logical_not(active))
    def _():
        obuf[...] = jnp.zeros_like(obuf)
        for copy in copies:
            copy.start()

    for copy in copies:
        copy.wait()


def local(tables, wave, previous, potential, column_extent, metric, center, halfwidth):
    any_spec = pl.BlockSpec(memory_space=pltpu.HBM)
    vmem_spec = pl.BlockSpec(memory_space=pltpu.VMEM)
    smem_spec = pl.BlockSpec(memory_space=pltpu.SMEM)
    f32, bf16 = jnp.float32, jnp.bfloat16
    dma = pltpu.SemaphoreType.DMA
    packed = pl.pallas_call(
        kernel,
        out_shape=pltpu.VMEM((BANDS, 4, KEPT, N), f32),
        in_specs=[any_spec] * 5 + [smem_spec] * 2 + [any_spec] * 6,
        out_specs=vmem_spec,
        scratch_shapes=[
            pltpu.VMEM((4, N), jnp.int32),
            pltpu.SMEM((3,), f32),
            pltpu.VMEM((2, BANDS, 4, KEPT, N), f32),
            pltpu.VMEM((2, BANDS, 4, KEPT, N), f32),
            pltpu.VMEM((PLANES, N, N), f32),
            *[pltpu.VMEM(table.shape, bf16) for table in tables],
            pltpu.VMEM((32, N), f32),
            pltpu.VMEM((4, 2 * N, 2 * N), bf16),
            pltpu.VMEM((8 * N, N), f32),
            pltpu.VMEM((PLANES, N, N), f32),
            pltpu.VMEM((N, N), f32),
            pltpu.VMEM((N, N), f32),
            pltpu.VMEM((PLANES, BANDS, N, 2 * N), f32),
            pltpu.VMEM((N, 2 * N), bf16),
            pltpu.VMEM((N, 2 * N), bf16),
            pltpu.VMEM((PLANES, N, N), f32),
            pltpu.VMEM((8 * N, N), f32),
            pltpu.VMEM((BANDS, 4, KEPT, N), f32),
            dma((BANDS, 2)),
            dma((2,)),
            dma((6,)),
            dma((3,)),
            dma((PLANES,)),
            dma((PLANES,)),
            dma((PLANES,)),
            dma((PLANES,)),
            dma((9,)),
            dma((9,)),
            dma,
            dma,
            pltpu.SemaphoreType.REGULAR((10,)),
        ],
        compiler_params=pltpu.CompilerParams(
            collective_id=0, has_side_effects=True, vmem_limit_bytes=24 * 1024 * 1024
        ),
    )(
        *[
            pltpu.with_memory_space_constraint(value, pltpu.HBM)
            for value in (wave, previous, potential.reshape(32, N), column_extent, metric)
        ],
        center,
        halfwidth,
        *[pltpu.with_memory_space_constraint(table, pltpu.HBM) for table in tables],
    )
    return pl.pallas_call(
        expand,
        out_shape=jax.ShapeDtypeStruct(wave.shape, f32),
        in_specs=[vmem_spec],
        out_specs=any_spec,
        scratch_shapes=[pltpu.VMEM((2, BANDS, 4, N, N), f32), dma((BANDS,))],
        compiler_params=pltpu.CompilerParams(vmem_limit_bytes=8 * 1024 * 1024),
    )(packed)


def solution(mesh):
    tables = [jnp.asarray(table) for table in make_tables()]
    in_specs = (
        P(None, "band", "fft", None, None),
        P(None, "band", "fft", None, None),
        P("band", "fft", None),
        P("fft", None),
        P(),
        P(),
        P(),
    )
    out_specs = P(None, "band", "fft", None, None)
    return jax.shard_map(
        functools.partial(local, tables), mesh=mesh, in_specs=in_specs, out_specs=out_specs, check_vma=False
    )
```

```python
import functools
import math

import jax
import jax.numpy as jnp
import numpy as np
from jax import lax
from jax.experimental import pallas as pl
from jax.experimental.pallas import tpu as pltpu
from jax.sharding import PartitionSpec as P

N = 128
KEPT = 64
HALF = KEPT // 2
FFT = 32
ACTIVE = 16
BANDS = 2
PLANES = 5
FEW = 3
FIRST = (0,)
MESSAGES = 3 * (FFT - 1) + 2 * (ACTIVE - 1)
MESH = pl.DeviceIdType.MESH


def kept_indices():
    return np.concatenate([np.arange(HALF), np.arange(N - HALF, N)])


def cos_sin(rows, cols):
    angles = (np.outer(rows, cols) % N) * (2.0 * math.pi / N)
    return np.cos(angles), np.sin(angles)


def split(table):
    high = table.astype(jnp.bfloat16)
    low = (table - high.astype(np.float64)).astype(jnp.bfloat16)
    return high, low


def stacked(cosine, sine):
    cos_high, cos_low = split(cosine)
    sin_high, sin_low = split(sine)
    zero = np.zeros_like(cos_low)
    return np.concatenate(
        [
            np.concatenate([cos_high, cos_high], axis=1),
            np.concatenate([sin_high, sin_high], axis=1),
            np.concatenate([cos_low, zero], axis=1),
            np.concatenate([sin_low, zero], axis=1),
        ],
        axis=0,
    )


def make_tables():
    grid = np.arange(N)
    kept = kept_indices()
    slots = np.arange(ACTIVE)
    first_gx = 4 * np.where(slots < ACTIVE // 2, slots, slots + FFT - ACTIVE)

    cosine, sine = cos_sin(grid, kept)
    high, low = split(np.concatenate([cosine, sine], axis=1))
    zero = np.zeros_like(low)
    inverse_z = np.concatenate([np.concatenate([high, high], axis=1), np.concatenate([low, zero], axis=1)], axis=0)

    lanes = np.arange(N)
    natural = (lanes < HALF) | (lanes >= N - HALF)
    gy = np.where(natural, lanes, (lanes + KEPT) % N)
    cosine, sine = cos_sin(gy, grid)
    pick = natural[:, None]
    table = np.concatenate([np.where(pick, cosine, -sine), np.where(pick, sine, cosine)], axis=1)
    high, low = split(table)
    inverse_y = np.concatenate([high, high, low], axis=0)

    order = (first_gx[:, None] + np.arange(4)[None, :]).reshape(-1)
    cosine, sine = cos_sin(grid, order)
    cos_high, cos_low = split(cosine)
    sin_high, sin_low = split(sine)
    zero = np.zeros_like(cos_low)
    inverse_x = np.concatenate(
        [
            np.concatenate([cos_high, sin_high, cos_high, sin_high], axis=1),
            np.concatenate([cos_low, sin_low, zero, zero], axis=1),
        ],
        axis=0,
    )

    cosine, sine = cos_sin(order, grid)
    forward_x = stacked(cosine / N, sine / N)

    cosine, sine = cos_sin(grid, gy)
    pick = natural[None, :]
    table = np.concatenate([np.where(pick, cosine, -sine), np.where(pick, sine, cosine)], axis=0) / N
    forward_y = np.concatenate(split(table), axis=1)

    cosine, sine = cos_sin(kept, grid)
    forward_z = stacked(cosine / N, sine / N)
    return np.concatenate([inverse_z, inverse_y, inverse_x, forward_x, forward_y, forward_z], axis=0)


def halves(value):
    high = value.astype(jnp.bfloat16)
    low = (value - high.astype(jnp.float32)).astype(jnp.bfloat16)
    return high, low


def dot(left, right):
    return jnp.dot(left, right, preferred_element_type=jnp.float32)


def kernel(
    wave,
    previous,
    potential,
    extent_hbm,
    metric_hbm,
    center,
    halfwidth,
    tables_hbm,
    out,
    extent,
    metric,
    wbuf,
    pbuf,
    vbuf,
    tables,
    vown,
    zboth,
    sbuf,
    rbuf,
    yre,
    yim,
    fbuf,
    qhigh,
    qlow,
    gbuf,
    hbuf,
    base,
    wsem,
    psem,
    tsem,
    lsem,
    fsend,
    frecv,
    gsend,
    grecv,
    vsend,
    vrecv,
    erecv,
    ready,
):
    me = lax.axis_index("fft")
    band = lax.axis_index("band")
    my_x, my_z = lax.div(band, 4), lax.rem(band, 4)
    my_y, my_low = lax.div(me, 4), lax.rem(me, 4)
    active = jnp.logical_or(me < ACTIVE // 2, me >= FFT - ACTIVE // 2)
    slot = jnp.where(me < ACTIVE // 2, me, me - (FFT - ACTIVE))
    lows = [my_low] + [lax.rem(my_low + i, 4) for i in (1, 2, 3)]
    rows_of_peers = [(lax.rem(my_y + dy, 8), lows) for dy in (4, 3, 5, 2, 6, 1, 7)] + [(my_y, lows[1:])]
    z_peers = [lax.rem(my_z + d, 4) for d in (2, 1, 3)]
    x_peers = [lax.rem(my_x + d, 4) for d in (2, 1, 3)]

    def hello(semaphore, where):
        pl.semaphore_signal(semaphore, inc=1, device_id=where, device_id_type=MESH)

    def wait_for(semaphore, count):
        @pl.when(count > 0)
        def _():
            pl.semaphore_wait(semaphore, count)

    def turn_of(y, place):
        usual = 4 * jnp.where(y < 4, y, 11 - y) + place
        return jnp.where(jnp.logical_and(band == 0, usual == 0), FFT, usual)

    my_turn = turn_of(my_y, my_low)
    earlier = jnp.where(band == 0, my_turn - 1, my_turn)
    z_shift = jnp.where(jnp.logical_and(me == 0, my_x == 0), 1, 0)
    x_shift = jnp.where(jnp.logical_and(me == 0, my_z == 0), 1, 0)

    def z_turn(z):
        return jnp.where(z < z_shift, 1, jnp.where(z == 1, 1 - z_shift, z))

    def x_turn(x):
        return jnp.where(x < x_shift, 3, x - x_shift)

    my_z_turn, my_x_turn = z_turn(my_z), x_turn(my_x)

    late = jnp.logical_and(band == 0, me == 0)
    side_2 = jnp.logical_and(my_y >= 2, my_y < 4)
    side_6 = my_y >= 6
    later_rows = jnp.where(late, 0, jnp.where(my_y == 0, 12, jnp.where(my_y == 1, 8, jnp.where(my_y == 7, 4, 0))))

    my_row = jnp.where(my_y < 4, my_y, 11 - my_y)
    y_order = (4, 5, 6, 3, 7, 2, 1, 0)

    def greet(semaphore, later):
        def to(y, line, core, semaphore):
            place = 2 * line + core
            if y == 0 and core == 0 and not later:

                @pl.when(jnp.logical_or(band != 0, line != 0))
                def _():
                    hello(semaphore, {"fft": y * 4 + place})
            else:
                hello(semaphore, {"fft": y * 4 + place})

        for y in y_order:
            y_row = y if y < 4 else 11 - y
            near = y_row > my_row if later else y_row < my_row
            if later and y >= 6:
                near = near & jnp.logical_not(side_2)
            if not later and 2 <= y < 4:
                near = near & jnp.logical_not(side_6)

            def row(semaphore):
                for line in range(2):
                    for core in range(2):
                        to(y, line, core, semaphore)

            if later or 2 <= y < 6:
                pl.when(near)(lambda: row(semaphore))
            else:
                pl.when(near & active)(lambda: row(ready.at[4]))
                pl.when(near & jnp.logical_not(active))(lambda: row(semaphore))

        for place in range(4):

            @pl.when(place > my_low if later else place < my_low)
            def _():
                if place > 0:
                    hello(semaphore, {"fft": my_y * 4 + place})
                else:

                    @pl.when(jnp.logical_or(band != 0, my_y > 0))
                    def _():
                        hello(semaphore, {"fft": my_y * 4})

    def greet_all(semaphore):
        for y in range(FFT // 4):
            for place in range(4):
                if y + place > 0:
                    hello(semaphore, {"fft": y * 4 + place})

    def is_late_row(y):
        return jnp.logical_and(band == 0, y == 0)

    load_v = pltpu.make_async_copy(potential, vown, lsem.at[0])
    load_v.start()
    barrier = pltpu.get_barrier_semaphore()
    direct = jnp.logical_not(active)
    early = jnp.logical_and(direct, my_z < 2)
    tardy = jnp.logical_and(direct, my_z >= 2)

    @pl.when(jnp.logical_not(late))
    def _():
        greet(barrier, True)

    @pl.when(jnp.logical_and(band == 0, me > 0))
    def _():
        hello(barrier, {"fft": 0})

    @pl.when(my_z < 2)
    def _():
        for z in (2, 3):
            for x in x_peers:
                hello(barrier, {"band": x * 4 + z})

    for z in z_peers:

        @pl.when(z_turn(z) > my_z_turn)
        def _():
            hello(barrier, {"band": my_x * 4 + z})

    for x in x_peers:

        @pl.when(x_turn(x) > my_x_turn)
        def _():
            hello(barrier, {"band": x * 4 + my_z})

    def wave_copies(b):
        return [
            pltpu.make_async_copy(
                wave.at[:, b, :, pl.ds(h * (N - HALF), HALF), :],
                wbuf.at[:, b, :, pl.ds(h * HALF, HALF), :],
                wsem,
            )
            for h in range(2)
        ]

    previous_copies = [
        pltpu.make_async_copy(
            previous.at[:, :, :, pl.ds(h * (N - HALF), HALF), :],
            pbuf.at[:, :, :, pl.ds(h * HALF, HALF), :],
            psem,
        )
        for h in range(2)
    ]
    small_refs = ((extent_hbm, extent), (metric_hbm, metric))
    small_copies = [pltpu.make_async_copy(a, b, lsem.at[i + 1]) for i, (a, b) in enumerate(small_refs)]
    starts = (0, 256, 640, 896, 1152, 1408, 1664)
    iz, iy, ix, fx, fy, fz = [tables.at[pl.ds(a, b - a), :] for a, b in zip(starts[:-1], starts[1:], strict=True)]
    table_copies = [
        pltpu.make_async_copy(tables_hbm.at[pl.ds(a, b - a), :], tables.at[pl.ds(a, b - a), :], tsem.at[i])
        for i, (a, b) in enumerate(((0, 256), (256, 1664)))
    ]

    for copy in small_copies:
        copy.start()

    @pl.when(active)
    def _():
        for b in range(BANDS):
            for copy in wave_copies(b):
                copy.start()

    for copy in table_copies:
        copy.start()

    @pl.when(active)
    def _():
        for copy in previous_copies:
            copy.start()

    row = lax.broadcasted_iota(jnp.int32, (KEPT, N), 0)
    lane = lax.broadcasted_iota(jnp.int32, (KEPT, N), 1)
    natural = jnp.logical_or(lane < HALF, lane >= N - HALF)
    signed_gz = jnp.where(row < HALF, row, row - KEPT)
    place_gy = jnp.where(natural, lane, jnp.where(lane < KEPT, lane + KEPT, lane - KEPT))
    signed_gy = jnp.where(place_gy < N // 2, place_gy, place_gy - N)
    turn_sign = jnp.where(natural, -1.0, 1.0).astype(jnp.float32)

    def is_active(y):
        return jnp.logical_or(y < 2, y >= 6)

    def partner(y):
        return lax.rem(jnp.where(jnp.logical_or(y < 2, jnp.logical_or(y == 4, y == 5)), y + 2, y + 6), 8)

    def plane_of(y, place, c):
        if c < 4:
            return 4 * (y * 4 + place) + c
        if isinstance(y, int):
            return 4 * ((y + 2 if y < 2 else y - 2) * 4 + place) + 3
        return 4 * (partner(y) * 4 + place) + 3

    def keep_of(j):
        return (jnp.abs(signed_gz) <= extent[pl.ds(j, 1), :]).astype(jnp.float32)

    def both_parts(keep, real, imag):
        return keep * real + pltpu.roll(keep * imag, KEPT, axis=1)

    def to_planes():
        pltpu.make_async_copy(wbuf, wbuf, wsem).wait()
        for j in range(4):
            keep = keep_of(j)
            for b in range(BANDS):
                packed = both_parts(keep, wbuf[0, b, j], wbuf[1, b, j])
                turned = pltpu.roll(packed, KEPT, axis=1) * turn_sign
                for t, part in enumerate((packed, turned)):
                    high, low = halves(part)
                    zboth[j, t * KEPT : (t + 1) * KEPT, b * N : (b + 1) * N] = high
                    zboth[j, N + t * KEPT : N + (t + 1) * KEPT, b * N : (b + 1) * N] = low
            both = dot(iz[...], zboth[j])
            both = both[:N] + both[N:]
            for b in range(BANDS):
                sbuf[pl.ds(2 * j + b, N, stride=8), :] = both[:, b * N : (b + 1) * N]
        for c in range(PLANES):
            mine = sbuf[pl.ds(pl.multiple_of(plane_of(my_y, my_low, c) * 8, 8), 8), :]
            rbuf[c, pl.ds(pl.multiple_of(slot * 8, 8), 8), :] = mine

    def scale():
        return jnp.full((1, N), 2.0, jnp.float32) / jnp.full((1, N), halfwidth[0], jnp.float32)

    def the_rest():
        pltpu.make_async_copy(pbuf, pbuf, psem).wait()
        step_z = (2.0 * math.pi / N) * signed_gz.astype(jnp.float32)
        step_y = (2.0 * math.pi / N) * signed_gy.astype(jnp.float32)
        plane_kinetic = metric[2] * (step_z * step_z) + metric[1] * (step_y * step_y)
        factor = scale()
        for j in range(4):
            gx = me * 4 + j
            signed_gx = jnp.where(gx < N // 2, gx, gx - N).astype(jnp.float32)
            step_x = (2.0 * math.pi / N) * signed_gx
            weight = factor * (0.5 * (metric[0] * (step_x * step_x) + plane_kinetic) - center[0])
            keep = keep_of(j)
            for b in range(BANDS):
                coefficient = both_parts(keep, wbuf[0, b, j], wbuf[1, b, j])
                base[b, j] = weight * coefficient - both_parts(keep, pbuf[0, b, j], pbuf[1, b, j])

    def send_plane(c, y, place):
        pltpu.make_async_remote_copy(
            src_ref=sbuf.at[pl.ds(pl.multiple_of(plane_of(y, place, c) * 8, 8), 8), :],
            dst_ref=rbuf.at[c, pl.ds(pl.multiple_of(slot * 8, 8), 8), :],
            send_sem=fsend,
            recv_sem=frecv.at[c],
            device_id={"fft": y * 4 + place},
            device_id_type=MESH,
        ).start()

    def to_others(y, send):
        @pl.when(my_y == y)
        def _():
            for place in lows[1:]:
                send(y, place)

        @pl.when(my_y != y)
        def _():
            for place in lows:
                send(y, place)

    def send_row(c, y):
        def unless_late(place):
            @pl.when(jnp.logical_and(place > 0, y * 4 + place != me))
            def _():
                send_plane(c, y, place)

        def send(y, place):
            send_plane(c, y, place)

        if y > 0:
            to_others(y, send)
        else:

            @pl.when(band == 0)
            def _():
                for place in lows:
                    unless_late(place)

            @pl.when(band != 0)
            def _():
                to_others(y, send)

    def send_rows(planes, rows):
        for c in planes:
            for y in rows:
                if 2 <= y < 6:
                    for place in lows:
                        send_plane(c, y, place)
                else:
                    send_row(c, y)

    def send_columns(c):
        plane = plane_of(my_y, my_low, c)

        def send(y, place):
            first = (y if y < 2 else y - 4) * 4
            pltpu.make_async_remote_copy(
                src_ref=gbuf.at[c, pl.ds(pl.multiple_of((first + place) * 8, 8), 8), :],
                dst_ref=hbuf.at[pl.ds(pl.multiple_of(plane * 8, 8), 8), :],
                send_sem=gsend,
                recv_sem=grecv,
                device_id={"fft": y * 4 + place},
                device_id_type=MESH,
            ).start()

        @pl.when(active)
        def _():
            for y in (0, 1, 7, 6):
                to_others(y, send)

        if c < FEW:

            @pl.when(jnp.logical_not(active))
            def _():
                for y in (0, 1, 7, 6):
                    for place in lows:
                        send(y, place)

    def awaited(ref, send, recv):
        return pltpu.make_async_remote_copy(
            src_ref=ref, dst_ref=ref, send_sem=send, recv_sem=recv, device_id={"fft": me}, device_id_type=MESH
        )

    def send_v(where, phase, peer):
        pltpu.make_async_remote_copy(
            src_ref=where,
            dst_ref=where,
            send_sem=vsend,
            recv_sem=vrecv.at[phase],
            device_id={"band": peer},
            device_id_type=MESH,
        ).start()

    my_rows = pl.ds(pl.multiple_of(band * 8, 8), 8)

    def v_part(planes, rows):
        return vbuf.at[pl.ds(0, planes), rows, :]

    def v_rows(z):
        return pl.ds(pl.multiple_of(my_x * 32 + z * 8, 8), 8)

    def for_kind(function):
        pl.when(active)(lambda: function(4))
        pl.when(jnp.logical_not(active))(lambda: function(FEW))

    def takes_z(z):
        return jnp.logical_not(jnp.logical_and(tardy, z < 2))

    def send_v_along_z(z, turn):
        @pl.when(takes_z(z))
        def _():
            for_kind(lambda planes: send_v(v_part(planes, my_rows), turn, my_x * 4 + z))

    def v_along_z(planes, turn):
        return awaited(v_part(planes, pl.ds(0, 8)), vsend, vrecv.at[turn])

    def send_v_along_x(z):
        for x in x_peers:
            for_kind(lambda planes: send_v(v_part(planes, v_rows(z)), 4, x * 4 + my_z))

    def send_v_directly(part, phase):
        for z in range(2):
            for x in x_peers + [my_x]:
                send_v(part, phase, x * 4 + z)

    def v_wait(planes, phase, rows):
        return awaited(v_part(planes, pl.ds(0, rows)), vsend, vrecv.at[phase])

    def v_last(phase, rows):
        return awaited(vbuf.at[4, pl.ds(0, rows), :], vsend, vrecv.at[phase])

    v_handed = pltpu.make_async_remote_copy(
        src_ref=vbuf.at[3, my_rows, :],
        dst_ref=vbuf.at[4, my_rows, :],
        send_sem=vsend,
        recv_sem=erecv,
        device_id={"fft": partner(my_y) * 4 + my_low},
        device_id_type=MESH,
    )

    def field(c):
        with jax.named_scope(f"wait_planes{c}"):

            @pl.when(active)
            def _():
                awaited(rbuf.at[c, pl.ds(0, 8 * (ACTIVE - 1)), :], fsend, frecv.at[c]).wait_recv()

            if c < FEW:

                @pl.when(jnp.logical_not(active))
                def _():
                    awaited(rbuf.at[c], fsend, frecv.at[c]).wait_recv()

        high, low = halves(rbuf[c])
        plane = dot(jnp.concatenate([high, low, high], axis=1), iy[...])
        yre[...] = plane[:, :N]
        yim[...] = plane[:, N:]
        for b in range(BANDS):
            rh, rl = halves(yre[pl.ds(b, KEPT, stride=2), :])
            ih, il = halves(yim[pl.ds(b, KEPT, stride=2), :])
            right = jnp.concatenate(
                [
                    jnp.concatenate([rh, ih], axis=1),
                    jnp.concatenate([-ih, rh], axis=1),
                    jnp.concatenate([rl, il], axis=1),
                    jnp.concatenate([-il, rl], axis=1),
                ],
                axis=0,
            )
            both = dot(ix[...], right)
            fbuf[c, b] = both[:N] + both[N:]

    def back(c):
        if c == 0:
            with jax.named_scope("wait_v"):

                def arrived(planes):
                    @pl.when(early)
                    def _():
                        v_wait(planes, 4, 112).wait_recv()

                    @pl.when(jnp.logical_not(early))
                    def _():
                        v_wait(planes, 4, 96).wait_recv()

                for_kind(arrived)
        if c == 4:
            with jax.named_scope("wait_v4"):

                @pl.when(my_z < 2)
                def _():
                    v_last(6, 112).wait_recv()

                @pl.when(my_z >= 2)
                def _():
                    v_last(6, 96).wait_recv()

        local_v = vbuf[c]
        for b in range(BANDS):
            rh, rl = halves(fbuf[c, b, :, :N] * local_v)
            ih, il = halves(fbuf[c, b, :, N:] * local_v)
            right = jnp.concatenate(
                [jnp.concatenate([rh, ih], axis=1), jnp.concatenate([rl, il], axis=1)], axis=0
            )
            both = dot(fx[...], right)
            both = both[:N] + both[N:]
            cos_part, sin_part = both[:KEPT], both[KEPT:]
            rows = slice(b * KEPT, (b + 1) * KEPT)
            high, low = halves(cos_part[:, :N] + sin_part[:, N:])
            qhigh[rows, :N] = high
            qlow[rows, :N] = low
            high, low = halves(cos_part[:, N:] - sin_part[:, :N])
            qhigh[rows, N:] = high
            qlow[rows, N:] = low
        wide = dot(qhigh[...], fy[...])
        packed = wide[:, :N] + wide[:, N:] + dot(qlow[...], fy[:, :N])
        for b in range(BANDS):
            gbuf[c, pl.ds(b, KEPT, stride=2), :] = packed[b * KEPT : (b + 1) * KEPT]
        with jax.named_scope(f"send_columns{c}"):
            send_columns(c)

        def keep_mine():
            mine = gbuf[c, pl.ds(pl.multiple_of(slot * 8, 8), 8), :]
            hbuf[pl.ds(pl.multiple_of(plane_of(my_y, my_low, c) * 8, 8), 8), :] = mine

        if c < FEW:
            pl.when(active)(keep_mine)
        else:
            keep_mine()

    with jax.named_scope("barrier"):
        wait_for(barrier, earlier + my_z_turn + my_x_turn + jnp.where(my_z >= 2, 6, 0) - jnp.where(side_6, 8, 0))
        load_v.wait()
        for c in range(4):
            vbuf[c, my_rows, :] = vown[pl.ds(c, 8, stride=4), :]

    @pl.when(tardy)
    def _():
        send_v_directly(v_part(FEW, my_rows), 4)

    @pl.when(late)
    def _():
        greet_all(ready.at[2])

    @pl.when(jnp.logical_not(late))
    def _():
        greet(ready.at[1], False)

    waits_for_first = jnp.logical_and(band == 0, me == 8)

    @pl.when(jnp.logical_not(jnp.logical_or(active, waits_for_first)))
    def _():
        v_handed.start()


    for z in z_peers:

        @pl.when(z_turn(z) < my_z_turn)
        def _():
            hello(ready.at[4 + my_z_turn], {"band": my_x * 4 + z})
            send_v_along_z(z, my_z_turn)

    for x in x_peers:

        @pl.when(x_turn(x) < my_x_turn)
        def _():
            hello(ready.at[0], {"band": x * 4 + my_z})

    for copy in small_copies:
        copy.wait()
    table_copies[0].wait()

    @pl.when(active)
    def _():
        with jax.named_scope("planes"):
            to_planes()

        with jax.named_scope("send_first"):

            @pl.when(my_y == 1)
            def _():
                send_rows(FIRST, (0,))

            @pl.when(my_y == 7)
            def _():
                send_rows(FIRST, (1, 0))

            @pl.when(my_y == 6)
            def _():
                send_rows(FIRST, (1, 0, 7))

    def hand_on(z, later):
        @pl.when(active & (z_turn(z) > my_z_turn if later else z_turn(z) < my_z_turn) & jnp.logical_not((my_z >= 2) & (z < 2)))
        def _():
            send_v(vbuf.at[4, my_rows, :], 5, my_x * 4 + z)

    @pl.when(jnp.logical_and(active, jnp.logical_not(late)))
    def _():
        with jax.named_scope("wait_handed"):
            v_handed.wait_recv()
        for z in z_peers:
            hand_on(z, False)

        @pl.when(my_z >= 2)
        def _():
            send_v_directly(vbuf.at[4, my_rows, :], 6)

    def own_along_x():
        with jax.named_scope("wait_x"):
            wait_for(ready.at[0], 3 - my_x_turn)
        send_v_along_x(my_z)

    def z_of(turn):
        return jnp.abs(turn - z_shift) if turn < 2 else turn

    def reach_z(turn):
        @pl.when(turn > my_z_turn)
        def _():
            with jax.named_scope(f"wait_z{turn}"):
                pl.semaphore_wait(ready.at[4 + turn], 1)
            send_v_along_z(z_of(turn), my_z_turn)

            @pl.when(jnp.logical_not(late))
            def _():
                hand_on(z_of(turn), True)

    def forward_v(turn):
        @pl.when(turn != my_z_turn if turn < 2 else jnp.logical_and(turn != my_z_turn, jnp.logical_not(early)))
        def _():
            with jax.named_scope(f"wait_vz{turn}"):
                for_kind(lambda planes: v_along_z(planes, turn).wait_recv())
            send_v_along_x(z_of(turn))

    def know_late():
        @pl.when(jnp.logical_and(band == 0, me > 0))
        def _():
            with jax.named_scope("wait_late"):
                pl.semaphore_wait(ready.at[2], 1)

            @pl.when(me == 8)
            def _():
                v_handed.start()

            @pl.when(active)
            def _():
                for c in range(PLANES):
                    send_plane(c, 0, 0)

    @pl.when(active)
    def _():
        own_along_x()

    @pl.when(jnp.logical_not(active))
    def _():
        own_along_x()
        reach_z(1)
        forward_v(0)
        forward_v(1)
        know_late()
        reach_z(2)
        reach_z(3)
        forward_v(2)
        forward_v(3)

    with jax.named_scope("wait_rows"):
        wait_for(ready.at[4], later_rows)

    with jax.named_scope("send_rows"):

        @pl.when(my_y == 0)
        def _():
            send_rows(FIRST, (6, 7, 1))

        @pl.when(my_y == 1)
        def _():
            send_rows(FIRST, (6, 7))

        @pl.when(my_y == 7)
        def _():
            send_rows(FIRST, (6,))

    with jax.named_scope("wait_group"):
        wait_for(
            ready.at[1],
            jnp.where(late, 0, jnp.where(band == 0, FFT - 2, FFT - 1) - earlier - jnp.where(side_2, 8, 0) - later_rows),
        )

    @pl.when(my_y == 1)
    def _():
        for y in (7, 6):
            hello(ready.at[3], {"fft": y * 4 + my_low})

    with jax.named_scope("send"):

        rest = [c for c in range(PLANES) if c not in FIRST]

        def own_row(planes):
            for y in (0, 1, 6, 7):

                @pl.when(my_y == y)
                def _():
                    send_rows(planes, (y,))

        @pl.when(my_y < 2)
        def _():
            send_rows((0,), (4, 3, 5, 2))
            own_row(FIRST)
            send_rows((1,), (4, 3, 5, 2))
            send_rows(rest[:1], (6, 7, 1, 0))
            send_rows((2,), (4, 3, 5, 2))
            send_rows(rest[1:], (6, 7, 1, 0))

        @pl.when(side_6)
        def _():
            send_rows((0,), (4, 5))
            own_row(FIRST)
            pl.semaphore_wait(ready.at[3], 1)
            send_rows((0,), (3, 2))
            send_rows((1,), (3, 4, 2, 5))
            send_rows(rest[:1], (1, 0, 7, 6))
            send_rows((2,), (3, 4, 2, 5))
            send_rows(rest[1:], (1, 0, 7, 6))

    @pl.when(active)
    def _():
        reach_z(1)
        forward_v(0)
        forward_v(1)
        know_late()
        reach_z(2)
        reach_z(3)
        with jax.named_scope("the_rest"):
            the_rest()
        forward_v(2)
        forward_v(3)

        @pl.when(late)
        def _():
            v_handed.wait_recv()
            for z in z_peers:
                hand_on(z, False)
                hand_on(z, True)

    for copy in table_copies[1:]:
        copy.wait()

    def forward_last():
        with jax.named_scope("wait_vlast"):

            def forward(blocks):
                v_last(5, 8 * blocks - 8 if blocks > 2 else 8).wait_recv()
                for x in x_peers:
                    send_v(vbuf.at[4, pl.ds(pl.multiple_of(my_x * 32, 32), 8 * blocks), :], 6, x * 4 + my_z)

            pl.when(my_z < 2)(lambda: forward(2))
            pl.when(my_z >= 2)(lambda: forward(4))

    for c in range(FEW):
        field(c)
        back(c)
        if c == 0:
            pl.when(active)(forward_last)

    def peers_with(c):
        return FFT - 1 if c < FEW else ACTIVE - 1

    @pl.when(active)
    def _():
        for c in range(FEW, PLANES):
            field(c)
            back(c)
        factor = scale()
        with jax.named_scope("wait_columns"):
            awaited(hbuf.at[pl.ds(0, 8 * MESSAGES), :], gsend, grecv).wait_recv()
        for j in range(4):
            h0, l0 = halves(hbuf[pl.ds(2 * j, N, stride=8), :])
            h1, l1 = halves(hbuf[pl.ds(2 * j + 1, N, stride=8), :])
            right = jnp.concatenate(
                [jnp.concatenate([h0, h1], axis=1), jnp.concatenate([l0, l1], axis=1)], axis=0
            )
            both = dot(fz[...], right)
            both = both[:N] + both[N:]
            keep = keep_of(j)
            keep = keep + pltpu.roll(keep, KEPT, axis=1)
            for b in range(BANDS):
                cos_part = both[:KEPT, b * N : (b + 1) * N]
                sin_part = both[KEPT:, b * N : (b + 1) * N]
                applied = cos_part - turn_sign * pltpu.roll(sin_part, KEPT, axis=1)
                out[b, j] = keep * (factor * applied) + base[b, j]

    with jax.named_scope("wait_sends"):

        def v_sent(rows):
            awaited(hbuf.at[pl.ds(0, rows), :], vsend, erecv).wait_send()

        @pl.when(active)
        def _():
            awaited(sbuf.at[pl.ds(0, 8 * MESSAGES), :], fsend, erecv).wait_send()
            awaited(gbuf.at[:, pl.ds(0, 8 * (ACTIVE - 1)), :], gsend, erecv).wait_send()
            pl.when(my_z < 2)(lambda: v_sent(552))
            pl.when(my_z >= 2)(lambda: v_sent(648))

        @pl.when(jnp.logical_not(active))
        def _():
            awaited(gbuf.at[pl.ds(0, FEW), :, :], gsend, erecv).wait_send()
            pl.when(early)(lambda: v_sent(224))
            pl.when(tardy)(lambda: v_sent(512))


def expand(packed, out, obuf, sem):
    me = lax.axis_index("fft")
    active = jnp.logical_or(me < ACTIVE // 2, me >= FFT - ACTIVE // 2)
    lane = lax.broadcasted_iota(jnp.int32, (KEPT, N), 1)
    natural = jnp.logical_or(lane < HALF, lane >= N - HALF)
    copies = [pltpu.make_async_copy(obuf.at[:, b], out.at[:, b], sem.at[b]) for b in range(BANDS)]

    @pl.when(active)
    def _():
        for b in range(BANDS):
            for j in range(4):
                both = packed[b, j]
                for t, part in enumerate((both, pltpu.roll(both, KEPT, axis=1))):
                    part = jnp.where(natural, part, 0.0)
                    obuf[t, b, j, :HALF, :] = part[:HALF]
                    obuf[t, b, j, HALF : N - HALF, :] = jnp.zeros((KEPT, N), jnp.float32)
                    obuf[t, b, j, N - HALF :, :] = part[HALF:]
            copies[b].start()

    @pl.when(jnp.logical_not(active))
    def _():
        obuf[...] = jnp.zeros_like(obuf)
        for copy in copies:
            copy.start()

    for copy in copies:
        copy.wait()


def local(tables, wave, previous, potential, column_extent, metric, center, halfwidth):
    any_spec = pl.BlockSpec(memory_space=pltpu.HBM)
    vmem_spec = pl.BlockSpec(memory_space=pltpu.VMEM)
    smem_spec = pl.BlockSpec(memory_space=pltpu.SMEM)
    f32, bf16 = jnp.float32, jnp.bfloat16
    dma = pltpu.SemaphoreType.DMA
    packed = pl.pallas_call(
        kernel,
        out_shape=pltpu.VMEM((BANDS, 4, KEPT, N), f32),
        in_specs=[any_spec] * 5 + [smem_spec] * 2 + [any_spec],
        out_specs=vmem_spec,
        scratch_shapes=[
            pltpu.VMEM((4, N), jnp.int32),
            pltpu.SMEM((3,), f32),
            pltpu.VMEM((2, BANDS, 4, KEPT, N), f32),
            pltpu.VMEM((2, BANDS, 4, KEPT, N), f32),
            pltpu.VMEM((PLANES, N, N), f32),
            pltpu.VMEM(tables.shape, bf16),
            pltpu.VMEM((32, N), f32),
            pltpu.VMEM((4, 2 * N, 2 * N), bf16),
            pltpu.VMEM((8 * N, N), f32),
            pltpu.VMEM((PLANES, N, N), f32),
            pltpu.VMEM((N, N), f32),
            pltpu.VMEM((N, N), f32),
            pltpu.VMEM((PLANES, BANDS, N, 2 * N), f32),
            pltpu.VMEM((N, 2 * N), bf16),
            pltpu.VMEM((N, 2 * N), bf16),
            pltpu.VMEM((PLANES, N, N), f32),
            pltpu.VMEM((8 * N, N), f32),
            pltpu.VMEM((BANDS, 4, KEPT, N), f32),
            dma,
            dma,
            dma((2,)),
            dma((3,)),
            dma,
            dma((PLANES,)),
            dma,
            dma,
            dma,
            dma((7,)),
            dma,
            pltpu.SemaphoreType.REGULAR((8,)),
        ],
        compiler_params=pltpu.CompilerParams(
            collective_id=0, has_side_effects=True, vmem_limit_bytes=24 * 1024 * 1024
        ),
    )(
        *[
            pltpu.with_memory_space_constraint(value, pltpu.HBM)
            for value in (wave, previous, potential.reshape(32, N), column_extent, metric)
        ],
        center,
        halfwidth,
        pltpu.with_memory_space_constraint(tables, pltpu.HBM),
    )
    return pl.pallas_call(
        expand,
        out_shape=jax.ShapeDtypeStruct(wave.shape, f32),
        in_specs=[vmem_spec],
        out_specs=any_spec,
        scratch_shapes=[pltpu.VMEM((2, BANDS, 4, N, N), f32), dma((BANDS,))],
        compiler_params=pltpu.CompilerParams(vmem_limit_bytes=8 * 1024 * 1024),
    )(packed)


def solution(mesh):
    tables = jnp.asarray(make_tables())
    in_specs = (
        P(None, "band", "fft", None, None),
        P(None, "band", "fft", None, None),
        P("band", "fft", None),
        P("fft", None),
        P(),
        P(),
        P(),
    )
    out_specs = P(None, "band", "fft", None, None)
    return jax.shard_map(
        functools.partial(local, tables), mesh=mesh, in_specs=in_specs, out_specs=out_specs, check_vma=False
    )
```
